256 devices in a mesh: row: 32 (over y, z), col: 8 (over x, core).
Axes of the slice: x: 4, y: 4, z: 8, core: 2. Of those that a mesh axis runs over, the one named last changes fastest.
Arguments:
- weights: bfloat16 [2, 8192, 8192], P(None, 'row', 'col'), may hold values from -0.0625 to 0.0625
- preact: float32 [2, 2, 8192], P(None, None, 'row'), may hold values from -2.5 to 2.5
- panel: bfloat16 [2, 64, 8192], P(None, None, 'col'), may hold values from -6 to 6
Outputs:
- basis_out: float32 [2, 64, 8192], P(None, None, 'col')
The draws below stay inside these ranges and needn't reach their ends.
All inputs are finite; a program needn't handle non-finite values.
Results may differ from the reference program's by a relative error of at most 0.035.
Values may be sent and summed in bfloat16 or wider, within the bound.
No kernel may reach another device: no remote copies, remote signals or barrier semaphores. Data moves between devices by JAX's collectives and lax.ppermute only.
A program may use at most 64 MiB of HBM per device.

```python
from functools import partial
import jax
import jax.numpy as jnp
from jax import lax

WIDTH = 8192
RANK = 64
LAYERS = 2
ITERS = 2
INPUTS = 2
N_ROW = 32
N_COL = 8


def block_levels(key, shape, split, low, top_value):
    def one(position, parts):
        draws = jax.random.uniform(jax.random.fold_in(jax.random.fold_in(key, 6), position), (parts,), jnp.float32, low / len(split), top_value / len(split))
        return jnp.repeat(jnp.exp(draws), shape[position] // parts).reshape((-1,) + (1,) * (len(shape) - position - 1))

    gain = one(*split[0])
    for cut in split[1:]:
        gain = gain * one(*cut)
    return gain


def scatter_about(key, shape, spread, most, shards=(), held_as=jnp.bfloat16):
    factor_of = block_levels(key, shape, shards, -0.22, 0.18) if shards else 1.0
    drawn = jax.random.normal(key, shape, jnp.float32) * spread * factor_of
    return jnp.minimum(jnp.maximum(drawn, -most), most).astype(held_as)


def setup_inputs(seed: int = 0) -> dict:
    keys = jax.random.split(jax.random.key(seed), 4)
    return {
        "weights": scatter_about(keys[0], (LAYERS, WIDTH, WIDTH), WIDTH ** -0.5, 0.0625, ((1, 32), (2, 8))),
        "preact": scatter_about(keys[1], (INPUTS, LAYERS, WIDTH), 0.8, 2.5, ((2, 32),), jnp.float32),
        "panel": scatter_about(keys[2], (INPUTS, RANK, WIDTH), 1.0, 6.0, ((2, 8),)),
    }


def forward_layer(values, weight):
    inputs, rows, width = values.shape
    blocks = values.astype(jnp.float32).reshape(inputs, rows, N_COL, width // N_COL)
    weight_blocks = weight.astype(jnp.float32).reshape(width, N_COL, width // N_COL)
    partials = jnp.einsum('bkci,oci->cbko', blocks, weight_blocks, precision=lax.Precision.HIGHEST)
    rounded = lax.optimization_barrier(partials.astype(jnp.bfloat16))
    return jnp.sum(rounded.astype(jnp.float32), axis=0)

def backward_layer(values, weight):
    inputs, rows, width = values.shape
    blocks = values.astype(jnp.float32).reshape(inputs, rows, N_ROW, width // N_ROW)
    weight_blocks = weight.astype(jnp.float32).reshape(N_ROW, width // N_ROW, width)
    partials = jnp.einsum('bkro,roi->rbki', blocks, weight_blocks, precision=lax.Precision.HIGHEST)
    rounded = lax.optimization_barrier(partials.astype(jnp.bfloat16))
    return jnp.sum(rounded.astype(jnp.float32), axis=0)

def reference(weights, preact, panel):
    slopes = 1.0 - jnp.tanh(preact) ** 2
    current = panel
    basis_out = panel.astype(jnp.float32)
    for iteration in range(ITERS):
        forward = current
        for layer_at in range(LAYERS):
            summed = forward_layer(forward, weights[layer_at])
            forward = (slopes[:, layer_at, None, :] * summed).astype(jnp.bfloat16)
        cotangent = forward
        for layer_at in reversed(range(LAYERS)):
            weighted = (slopes[:, layer_at, None, :] * cotangent.astype(jnp.float32)).astype(jnp.bfloat16)
            cotangent = backward_layer(weighted, weights[layer_at]).astype(jnp.bfloat16)
        image_panel = cotangent.astype(jnp.float32)
        gram_sum = jnp.einsum('bkw,bjw->bkj', image_panel, image_panel, precision=lax.Precision.HIGHEST)
        factor = jnp.linalg.cholesky(gram_sum / WIDTH)
        basis_out = jax.vmap(partial(jax.scipy.linalg.solve_triangular, lower=True))(factor, image_panel)
        current = basis_out.astype(jnp.bfloat16)
    return basis_out
```

```python
import jax
import jax.numpy as jnp
from jax import lax
from jax.experimental import pallas as pl
from jax.experimental.pallas import tpu as pltpu
from jax.sharding import Mesh, PartitionSpec as P

WIDTH = 8192
ITERS = 2
BF16 = jnp.bfloat16
F32 = jnp.float32


def dot_t(a, w):
    return lax.dot_general(a, w, (((1,), (1,)), ((), ())), preferred_element_type=F32)


def dot_n(a, w):
    return lax.dot_general(a, w, (((1,), (0,)), ((), ())), preferred_element_type=F32)


def exchange(tiles, axis):
    return lax.all_to_all(tiles, axis, split_axis=0, concat_axis=0, tiled=True)


def to_all(x, axis, count):
    return exchange(jnp.broadcast_to(x[None], (count, *x.shape)), axis)


def total(tiles):
    return jnp.sum(tiles.astype(F32), axis=0)


def inverse_factor(gram):
    n = gram.shape[0]
    rows = lax.broadcasted_iota(jnp.int32, (n, n), 0)
    cols = lax.broadcasted_iota(jnp.int32, (n, n), 1)
    eye = (rows == cols).astype(F32)
    both = jnp.concatenate([eye, gram * (1.0 / WIDTH)], axis=1)
    row_of = lax.broadcasted_iota(jnp.int32, (n, 2 * n), 0)
    for j in range(n - 1):
        column = jnp.broadcast_to(both[:, n + j : n + j + 1], (n, 2 * n))
        pivot_row = both[j : j + 1, :] / column[j : j + 1, :]
        both = both - jnp.where(row_of > j, column, 0.0) * pivot_row
    pivots = jnp.sum(both[:, n:] * eye, axis=1, keepdims=True)
    return both[:, :n] / jnp.sqrt(pivots)


def exact_dot(a, b):
    return lax.dot_general(
        a, b, (((1,), (0,)), ((), ())), precision=lax.Precision.HIGHEST, preferred_element_type=F32
    )


def gram_of_parts(parts_ref, start, rank):
    parts = [parts_ref[i, :, start : start + 2 * rank].astype(F32) for i in range(parts_ref.shape[0])]
    summed = parts[0]
    for part in parts[1:]:
        summed = summed + part
    return summed[:, :rank] + summed[:, rank:]


def normalized_forward(arrived, slope, width):
    rank = arrived.shape[1]

    def kernel(arrived_ref, slope_ref, out_ref):
        inverse = inverse_factor(gram_of_parts(arrived_ref, width, rank))
        summed = arrived_ref[0, :, :width].astype(F32)
        for i in range(1, arrived_ref.shape[0]):
            summed = summed + arrived_ref[i, :, :width].astype(F32)
        out_ref[...] = (slope_ref[...] * exact_dot(inverse, summed)).astype(BF16)

    return pl.pallas_call(
        kernel, out_shape=jax.ShapeDtypeStruct((rank, width), BF16), name="normalized_forward"
    )(arrived, slope)


def normalized_panel(arrived, own, other):
    rank = arrived.shape[1]

    def kernel(arrived_ref, own_ref, other_ref, own_out, other_out):
        inverse = inverse_factor(gram_of_parts(arrived_ref, 0, rank))
        own_out[...] = exact_dot(inverse, own_ref[...].astype(F32))
        other_out[...] = exact_dot(inverse, other_ref[...].astype(F32))

    shape = jax.ShapeDtypeStruct(own.shape, F32)
    return pl.pallas_call(kernel, out_shape=(shape, shape), name="normalized_panel")(arrived, own, other)


def high_low(gram):
    high = lax.reduce_precision(gram, 8, 7)
    return jnp.concatenate([high.astype(BF16), (gram - high).astype(BF16)], axis=1)


def make(n_x, n_y, n_z):
    swap = [(i * n_x + j, j * n_x + i) for i in range(n_y) for j in range(n_x)]
    flip = [(0, 1), (1, 0)]

    def on_device(weights, preact, panel):
        core = lax.axis_index("core")
        first = core == 0
        inputs, rank, width_in = panel.shape
        width_row = weights.shape[1]
        w1_own, w2_own = weights[0], weights[1]

        partial_out = jnp.einsum("bki,oi->bko", panel, w1_own, preferred_element_type=F32)
        mine = jnp.where(first, partial_out[0], partial_out[1])
        theirs = jnp.where(first, partial_out[1], partial_out[0])
        summed_out = mine + lax.ppermute(theirs, "core", flip)

        slopes = 1.0 - jnp.tanh(jnp.where(first, preact[0], preact[1])) ** 2
        slope_1 = slopes[0:1]
        slope_2 = lax.ppermute(slopes[1:2], ("y", "x"), swap)
        w2_moved = lax.ppermute(w2_own, ("y", "x"), swap)
        w2_other = lax.ppermute(w2_moved, "core", flip)
        w2_low = jnp.where(first, w2_moved, w2_other)
        w2_high = jnp.where(first, w2_other, w2_moved)
        w2 = jnp.concatenate([w2_low, w2_high], axis=1)
        w1_other = lax.ppermute(w1_own, "core", flip)

        own = other = None
        for iteration in range(ITERS):
            if iteration == 0:
                forward = (slope_1 * total(to_all(summed_out.astype(BF16), "x", n_x))).astype(BF16)
            else:
                partial_out = dot_t(own, w1_own) + dot_t(other, w1_other)
                gram = dot_t(own, own) + dot_t(other, other)
                message = jnp.concatenate([partial_out.astype(BF16), high_low(gram)], axis=1)
                forward = normalized_forward(to_all(message, "x", n_x), slope_1, width_row)
            spread = to_all(forward, "z", n_z)
            spread = jnp.moveaxis(spread, 0, 1).reshape(rank, n_z * width_row)
            partial_out = dot_t(spread, w2)
            forward = (slope_2 * total(to_all(partial_out.astype(BF16), "y", n_y))).astype(BF16)
            weighted = (slope_2 * forward.astype(F32)).astype(BF16)
            partial_in = dot_n(weighted, w2).astype(BF16)
            blocks = jnp.moveaxis(partial_in.reshape(rank, n_z, width_row), 1, 0)
            summed = total(exchange(blocks, "z")).astype(BF16)
            cotangent = total(to_all(summed, "x", n_x)).astype(BF16)
            weighted = (slope_1 * cotangent.astype(F32)).astype(BF16)
            partial_in = jnp.concatenate([dot_n(weighted, w1_own), dot_n(weighted, w1_other)], axis=1)
            groups = rank // 8
            cuts = n_y * n_z // groups
            length = 2 * width_in // cuts
            pieces = partial_in.astype(BF16).reshape(groups, 8, cuts, length)
            pieces = jnp.moveaxis(pieces, 2, 1).reshape(groups * cuts, 8, length)
            piece = total(exchange(pieces, ("y", "z"))).astype(BF16)
            image = to_all(piece, ("y", "z"), groups * cuts).reshape(groups, cuts, 8, length)
            image = jnp.moveaxis(image, 1, 2).reshape(rank, 2 * width_in)
            own, other = image[:, :width_in], image[:, width_in:]
        gram = dot_t(own, own) + dot_t(other, other)
        basis_own, basis_other = normalized_panel(to_all(high_low(gram), "x", n_x), own, other)
        received = lax.ppermute(basis_other, "core", flip)
        return jnp.stack([jnp.where(first, basis_own, received), jnp.where(first, received, basis_own)])

    return on_device


def solution(mesh):
    n_x, n_y, n_z = 4, 4, 8
    fine = Mesh(mesh.devices.reshape(n_y, n_z, n_x, 2), ("y", "z", "x", "core"))
    return jax.shard_map(
        make(n_x, n_y, n_z),
        mesh=fine,
        in_specs=(P(None, ("y", "z"), ("x", "core")), P(None, None, ("y", "z")), P(None, None, ("x", "core"))),
        out_specs=P(None, None, ("x", "core")),
        check_vma=False,
    )
```

```python
import jax
import jax.numpy as jnp
from jax import lax
from jax.experimental import pallas as pl
from jax.experimental.pallas import tpu as pltpu
from jax.sharding import Mesh, PartitionSpec as P

WIDTH = 8192
ITERS = 2
BF16 = jnp.bfloat16
F32 = jnp.float32


def dot_t(a, w):
    return lax.dot_general(a, w, (((1,), (1,)), ((), ())), preferred_element_type=F32)


def dot_n(a, w):
    return lax.dot_general(a, w, (((1,), (0,)), ((), ())), preferred_element_type=F32)


def exchange(tiles, axis):
    return lax.all_to_all(tiles, axis, split_axis=0, concat_axis=0, tiled=True)


def to_all(x, axis, count):
    return exchange(jnp.broadcast_to(x[None], (count, *x.shape)), axis)


def total(tiles):
    return jnp.sum(tiles.astype(F32), axis=0)


def inverse_factor(gram):
    n = gram.shape[0]
    count = n // 8
    rows = lax.broadcasted_iota(jnp.int32, (n, n), 0)
    cols = lax.broadcasted_iota(jnp.int32, (n, n), 1)
    both = jnp.concatenate([(rows == cols).astype(F32), gram * (1.0 / WIDTH)], axis=1)
    blocks = [both[8 * i : 8 * i + 8] for i in range(count)]
    row_of = lax.broadcasted_iota(jnp.int32, (8, 2 * n), 0)
    done = []
    for k in range(count):
        live = range(k, count)
        columns = [
            {i: jnp.broadcast_to(blocks[i][:, n + 8 * k + t : n + 8 * k + t + 1], (8, 2 * n)) for i in live}
            for t in range(8)
        ]
        scale = jnp.zeros((8, 2 * n), F32)
        for t in range(8):
            inverse = 1.0 / columns[t][k][t : t + 1, :]
            scale = jnp.where(row_of == t, inverse, scale)
            factors = {i: columns[t][i] * inverse for i in live}
            factors[k] = jnp.where(row_of > t, factors[k], 0.0)
            for u in range(t + 1, 8):
                entry = columns[u][k][t : t + 1, :]
                for i in live:
                    columns[u][i] = columns[u][i] - factors[i] * entry
            pivot_row = blocks[k][t : t + 1, :]
            for i in live:
                blocks[i] = blocks[i] - factors[i] * pivot_row
        done.append(blocks[k] * jnp.sqrt(scale))
    return jnp.concatenate(done, axis=0)[:, :n]


def exact_dot(a, b):
    return lax.dot_general(
        a, b, (((1,), (0,)), ((), ())), precision=lax.Precision.HIGHEST, preferred_element_type=F32
    )


def gram_of_parts(parts_ref, start, rank):
    parts = [parts_ref[i, :, start : start + 2 * rank].astype(F32) for i in range(parts_ref.shape[0])]
    summed = parts[0]
    for part in parts[1:]:
        summed = summed + part
    return summed[:, :rank] + summed[:, rank:]


def normalized_forward(arrived, slope, width):
    rank = arrived.shape[1]

    def kernel(arrived_ref, slope_ref, out_ref):
        inverse = inverse_factor(gram_of_parts(arrived_ref, width, rank))
        summed = arrived_ref[0, :, :width].astype(F32)
        for i in range(1, arrived_ref.shape[0]):
            summed = summed + arrived_ref[i, :, :width].astype(F32)
        out_ref[...] = (slope_ref[...] * exact_dot(inverse, summed)).astype(BF16)

    return pl.pallas_call(
        kernel, out_shape=jax.ShapeDtypeStruct((rank, width), BF16), name="normalized_forward"
    )(arrived, slope)


def normalized_panel(arrived, own, other):
    rank = arrived.shape[1]

    def kernel(arrived_ref, own_ref, other_ref, own_out, other_out):
        inverse = inverse_factor(gram_of_parts(arrived_ref, 0, rank))
        own_out[...] = exact_dot(inverse, own_ref[...].astype(F32))
        other_out[...] = exact_dot(inverse, other_ref[...].astype(F32))

    shape = jax.ShapeDtypeStruct(own.shape, F32)
    return pl.pallas_call(kernel, out_shape=(shape, shape), name="normalized_panel")(arrived, own, other)


def high_low(gram):
    high = lax.reduce_precision(gram, 8, 7)
    return jnp.concatenate([high.astype(BF16), (gram - high).astype(BF16)], axis=1)


def make(n_x, n_y, n_z):
    swap = [(i * n_x + j, j * n_x + i) for i in range(n_y) for j in range(n_x)]
    flip = [(0, 1), (1, 0)]

    def on_device(weights, preact, panel):
        core = lax.axis_index("core")
        first = core == 0
        inputs, rank, width_in = panel.shape
        width_row = weights.shape[1]
        w1_own, w2_own = weights[0], weights[1]

        partial_out = jnp.einsum("bki,oi->bko", panel, w1_own, preferred_element_type=F32)
        mine = jnp.where(first, partial_out[0], partial_out[1])
        theirs = jnp.where(first, partial_out[1], partial_out[0])
        summed_out = mine + lax.ppermute(theirs, "core", flip)

        slopes = 1.0 - jnp.tanh(jnp.where(first, preact[0], preact[1])) ** 2
        slope_1 = slopes[0:1]
        slope_2 = lax.ppermute(slopes[1:2], ("y", "x"), swap)

        def moved(block):
            here = lax.ppermute(block, ("y", "x"), swap)
            there = lax.ppermute(here, "core", flip)
            return jnp.concatenate([jnp.where(first, here, there), jnp.where(first, there, here)], axis=1)

        half = width_row // 2
        w2_top = moved(w2_own[:half])
        w1_other = lax.ppermute(w1_own, "core", flip)

        own = other = None
        for iteration in range(ITERS):
            if iteration == 0:
                forward = (slope_1 * total(to_all(summed_out.astype(BF16), "x", n_x))).astype(BF16)
                forward, w2_rest = lax.optimization_barrier((forward, w2_own[half:]))
                w2 = jnp.concatenate([w2_top, moved(w2_rest)], axis=0)
            else:
                partial_out = dot_t(own, w1_own) + dot_t(other, w1_other)
                gram = dot_t(own, own) + dot_t(other, other)
                message = jnp.concatenate([partial_out.astype(BF16), high_low(gram)], axis=1)
                forward = normalized_forward(to_all(message, "x", n_x), slope_1, width_row)
            spread = to_all(forward, "z", n_z)
            spread = jnp.moveaxis(spread, 0, 1).reshape(rank, n_z * width_row)
            partial_out = dot_t(spread, w2)
            forward = (slope_2 * total(to_all(partial_out.astype(BF16), "y", n_y))).astype(BF16)
            weighted = (slope_2 * forward.astype(F32)).astype(BF16)
            partial_in = dot_n(weighted, w2).astype(BF16)
            blocks = jnp.moveaxis(partial_in.reshape(rank, n_z, width_row), 1, 0)
            summed = total(exchange(blocks, "z")).astype(BF16)
            cotangent = total(to_all(summed, "x", n_x)).astype(BF16)
            weighted = (slope_1 * cotangent.astype(F32)).astype(BF16)
            partial_in = jnp.concatenate([dot_n(weighted, w1_own), dot_n(weighted, w1_other)], axis=1)
            groups = rank // 8
            cuts = n_y * n_z // groups
            length = 2 * width_in // cuts
            pieces = partial_in.astype(BF16).reshape(groups, 8, cuts, length)
            pieces = jnp.moveaxis(pieces, 2, 1).reshape(groups * cuts, 8, length)
            piece = total(exchange(pieces, ("y", "z"))).astype(BF16)
            image = to_all(piece, ("y", "z"), groups * cuts).reshape(groups, cuts, 8, length)
            image = jnp.moveaxis(image, 1, 2).reshape(rank, 2 * width_in)
            own, other = image[:, :width_in], image[:, width_in:]
        gram = dot_t(own, own) + dot_t(other, other)
        basis_own, basis_other = normalized_panel(to_all(high_low(gram), "x", n_x), own, other)
        received = lax.ppermute(basis_other, "core", flip)
        at = lax.broadcasted_iota(jnp.int32, (inputs, rank, width_in), 0)
        return jnp.where(at == core, basis_own[None], received[None])

    return on_device


def solution(mesh):
    n_x, n_y, n_z = 4, 4, 8
    fine = Mesh(mesh.devices.reshape(n_y, n_z, n_x, 2), ("y", "z", "x", "core"))
    return jax.shard_map(
        make(n_x, n_y, n_z),
        mesh=fine,
        in_specs=(P(None, ("y", "z"), ("x", "core")), P(None, None, ("y", "z")), P(None, None, ("x", "core"))),
        out_specs=P(None, None, ("x", "core")),
        check_vma=False,
    )
```

```python
import jax
import jax.numpy as jnp
from jax import lax
from jax.experimental import pallas as pl
from jax.experimental.pallas import tpu as pltpu
from jax.sharding import Mesh, PartitionSpec as P


WIDTH = 8192
ITERS = 2
EARLY = 96
BF16 = jnp.bfloat16
F32 = jnp.float32


def dot_t(a, w):
    return lax.dot_general(a, w, (((1,), (1,)), ((), ())), preferred_element_type=F32)


def dot_n(a, w):
    return lax.dot_general(a, w, (((1,), (0,)), ((), ())), preferred_element_type=F32)


def exchange(tiles, axis):
    return lax.all_to_all(tiles, axis, split_axis=0, concat_axis=0, tiled=True)


def to_all(x, axis, count):
    return exchange(jnp.broadcast_to(x[None], (count, *x.shape)), axis)


def total(tiles):
    return jnp.sum(tiles.astype(F32), axis=0)


def inverse_factor(gram):
    n = gram.shape[0]
    count = n // 8
    rows = lax.broadcasted_iota(jnp.int32, (n, n), 0)
    cols = lax.broadcasted_iota(jnp.int32, (n, n), 1)
    both = jnp.concatenate([(rows == cols).astype(F32), gram * (1.0 / WIDTH)], axis=1)
    blocks = [both[8 * i : 8 * i + 8] for i in range(count)]
    row_of = lax.broadcasted_iota(jnp.int32, (8, 2 * n), 0)
    done = []
    for k in range(count):
        live = range(k, count)
        columns = [
            {i: jnp.broadcast_to(blocks[i][:, n + 8 * k + t : n + 8 * k + t + 1], (8, 2 * n)) for i in live}
            for t in range(8)
        ]
        scale = jnp.zeros((8, 2 * n), F32)
        for t in range(8):
            inverse = 1.0 / columns[t][k][t : t + 1, :]
            scale = jnp.where(row_of == t, inverse, scale)
            factors = {i: columns[t][i] * inverse for i in live}
            factors[k] = jnp.where(row_of > t, factors[k], 0.0)
            for u in range(t + 1, 8):
                entry = columns[u][k][t : t + 1, :]
                for i in live:
                    columns[u][i] = columns[u][i] - factors[i] * entry
            pivot_row = blocks[k][t : t + 1, :]
            for i in live:
                blocks[i] = blocks[i] - factors[i] * pivot_row
        done.append(blocks[k] * jnp.sqrt(scale))
    return jnp.concatenate(done, axis=0)[:, :n]


def exact_dot(a, b):
    return lax.dot_general(
        a, b, (((1,), (0,)), ((), ())), precision=lax.Precision.HIGHEST, preferred_element_type=F32
    )


def gram_of_parts(parts_ref, start, rank):
    parts = [parts_ref[i, :, start : start + 2 * rank].astype(F32) for i in range(parts_ref.shape[0])]
    summed = parts[0]
    for part in parts[1:]:
        summed = summed + part
    return summed[:, :rank] + summed[:, rank:]


def inverse_of(arrived, start):
    rank = arrived.shape[1]

    def kernel(arrived_ref, out_ref):
        out_ref[...] = inverse_factor(gram_of_parts(arrived_ref, start, rank))

    return pl.pallas_call(
        kernel,
        out_shape=jax.ShapeDtypeStruct((rank, rank), F32),
        cost_estimate=pl.CostEstimate(flops=60_000_000, bytes_accessed=200_000, transcendentals=0),
        name="inverse_of",
    )(arrived)


def normalized_weighted(arrived, inverse, slope):
    count, rank, width = arrived.shape

    def kernel(arrived_ref, inverse_ref, slope_ref, out_ref):
        summed = arrived_ref[0].astype(F32)
        for i in range(1, count):
            summed = summed + arrived_ref[i].astype(F32)
        forward = (slope_ref[...] * exact_dot(inverse_ref[...], summed)).astype(BF16)
        out_ref[...] = (slope_ref[...] * forward.astype(F32)).astype(BF16)

    return pl.pallas_call(
        kernel, out_shape=jax.ShapeDtypeStruct((rank, width), BF16), name="normalized_weighted"
    )(arrived, inverse, slope)


def normalized_panels(core, inverse, inverse_there, image, there):
    rank, width = there.shape

    def kernel(core_ref, inverse_ref, inverse_there_ref, image_ref, there_ref, out_ref):
        here_at = core_ref[0]
        here = exact_dot(inverse_ref[...], image_ref[:, :width].astype(F32))
        out_ref[pl.ds(here_at, 1)] = here[None]
        away = exact_dot(inverse_there_ref[...], there_ref[...].astype(F32))
        out_ref[pl.ds(1 - here_at, 1)] = away[None]

    whole = pl.BlockSpec(memory_space=pltpu.VMEM)
    return pl.pallas_call(
        kernel,
        in_specs=[pl.BlockSpec(memory_space=pltpu.SMEM), whole, whole, whole, whole],
        out_specs=whole,
        out_shape=jax.ShapeDtypeStruct((2, rank, width), F32),
        name="normalized_panels",
    )(core, inverse, inverse_there, image, there)


def high_low(gram):
    high = lax.reduce_precision(gram, 8, 7)
    return jnp.concatenate([high.astype(BF16), (gram - high).astype(BF16)], axis=1)


def make(n_x, n_y, n_z):
    swap = [(i * n_x + j, j * n_x + i) for i in range(n_y) for j in range(n_x)]
    flip = [(0, 1), (1, 0)]

    def on_device(weights, preact, panel):
        core = lax.axis_index("core")
        first = core == 0
        _, rank, width_in = panel.shape
        width_row = weights.shape[1]
        w1_own, w2_own = weights[0], weights[1]

        partial_out = jnp.einsum("bki,oi->bko", panel, w1_own, preferred_element_type=F32)
        mine = jnp.where(first, partial_out[0], partial_out[1])
        theirs = jnp.where(first, partial_out[1], partial_out[0])
        summed_out = mine + lax.ppermute(theirs, "core", flip)

        slopes = 1.0 - jnp.tanh(jnp.where(first, preact[0], preact[1])) ** 2
        slope_1 = slopes[0:1]
        slope_2 = lax.ppermute(slopes[1:2], ("y", "x"), swap)

        def moved(block):
            here = lax.ppermute(block, ("y", "x"), swap)
            there = lax.ppermute(here, "core", flip)
            return jnp.concatenate([jnp.where(first, here, there), jnp.where(first, there, here)], axis=1)

        w2 = jnp.concatenate([moved(w2_own[:EARLY]), moved(w2_own[EARLY:])], axis=0)
        w1_other = lax.ppermute(w1_own, "core", flip)

        image = inverse = None
        for iteration in range(ITERS):
            if iteration == 0:
                arrived = to_all(summed_out.astype(BF16), "x", n_x)
            else:
                own, other = image[:, :width_in], image[:, width_in:]
                partial_out = dot_t(own, w1_own) + dot_t(other, w1_other)
                gram = dot_t(own, own) + dot_t(other, other)
                message = jnp.concatenate([partial_out.astype(BF16), high_low(gram)], axis=1)
                arrived = to_all(message, "x", n_x)
                inverse = inverse_of(arrived, width_row)
            forward = (slope_1 * total(arrived[:, :, :width_row])).astype(BF16)
            spread = to_all(forward, "z", n_z)
            spread = jnp.moveaxis(spread, 0, 1).reshape(rank, n_z * width_row)
            partial_out = dot_t(spread, w2)
            arrived = to_all(partial_out.astype(BF16), "y", n_y)
            if inverse is None:
                forward = (slope_2 * total(arrived)).astype(BF16)
                weighted = (slope_2 * forward.astype(F32)).astype(BF16)
            else:
                weighted = normalized_weighted(arrived, inverse, slope_2)
            partial_in = dot_n(weighted, w2).astype(BF16)
            blocks = jnp.moveaxis(partial_in.reshape(rank, n_z, width_row), 1, 0)
            summed = total(exchange(blocks, "z")).astype(BF16)
            cotangent = total(to_all(summed, "x", n_x)).astype(BF16)
            weighted = (slope_1 * cotangent.astype(F32)).astype(BF16)
            partial_in = jnp.concatenate([dot_n(weighted, w1_own), dot_n(weighted, w1_other)], axis=1)
            groups = rank // 8
            cuts = n_y * n_z // groups
            length = 2 * width_in // cuts
            pieces = partial_in.astype(BF16).reshape(groups, 8, cuts, length)
            pieces = jnp.moveaxis(pieces, 2, 1).reshape(groups * cuts, 8, length)
            piece = total(exchange(pieces, ("y", "z"))).astype(BF16)
            image = to_all(piece, ("y", "z"), groups * cuts).reshape(groups, cuts, 8, length)
            image = jnp.moveaxis(image, 1, 2).reshape(rank, 2 * width_in)
        there = lax.ppermute(image[:, width_in:], "core", flip)
        gram = dot_t(image, image)
        inverse = inverse_of(to_all(high_low(gram), "x", n_x), 0)
        inverse_there = lax.ppermute(inverse, "core", flip)
        return normalized_panels(core.reshape(1).astype(jnp.int32), inverse, inverse_there, image, there)

    return on_device


def solution(mesh):
    n_x, n_y, n_z = 4, 4, 8
    fine = Mesh(mesh.devices.reshape(n_y, n_z, n_x, 2), ("y", "z", "x", "core"))
    on_device = make(n_x, n_y, n_z)

    return jax.shard_map(
        on_device,
        mesh=fine,
        in_specs=(P(None, ("y", "z"), ("x", "core")), P(None, None, ("y", "z")), P(None, None, ("x", "core"))),
        out_specs=P(None, None, ("x", "core")),
        check_vma=False,
    )
```

```python
import jax
import jax.numpy as jnp
from jax import lax
from jax.experimental import pallas as pl
from jax.experimental.pallas import tpu as pltpu
from jax.sharding import Mesh, PartitionSpec as P


WIDTH = 8192
ITERS = 2
BF16 = jnp.bfloat16
F32 = jnp.float32
WHOLE = pl.BlockSpec(memory_space=pltpu.VMEM)


def on_chip(x):
    return pltpu.with_memory_space_constraint(x, pltpu.VMEM)


def dot_t(a, w):
    return lax.dot_general(a, w, (((1,), (1,)), ((), ())), preferred_element_type=F32)


def dot_n(a, w):
    return lax.dot_general(a, w, (((1,), (0,)), ((), ())), preferred_element_type=F32)


def exchange(tiles, axis):
    return lax.all_to_all(tiles, axis, split_axis=0, concat_axis=0, tiled=True)


def to_all(x, axis, count):
    return exchange(jnp.broadcast_to(x[None], (count, *x.shape)), axis)


def total(tiles):
    return jnp.sum(tiles.astype(F32), axis=0)


def inverse_factor(gram):
    n = gram.shape[0]
    count = n // 8
    rows = lax.broadcasted_iota(jnp.int32, (n, n), 0)
    cols = lax.broadcasted_iota(jnp.int32, (n, n), 1)
    both = jnp.concatenate([(rows == cols).astype(F32), gram * (1.0 / WIDTH)], axis=1)
    blocks = [both[8 * i : 8 * i + 8] for i in range(count)]
    row_of = lax.broadcasted_iota(jnp.int32, (8, 2 * n), 0)
    done = []
    for k in range(count):
        live = range(k, count)
        columns = [
            {i: jnp.broadcast_to(blocks[i][:, n + 8 * k + t : n + 8 * k + t + 1], (8, 2 * n)) for i in live}
            for t in range(8)
        ]
        scale = jnp.zeros((8, 2 * n), F32)
        for t in range(8):
            inverse = 1.0 / columns[t][k][t : t + 1, :]
            scale = jnp.where(row_of == t, inverse, scale)
            factors = {i: columns[t][i] * inverse for i in live}
            factors[k] = jnp.where(row_of > t, factors[k], 0.0)
            for u in range(t + 1, 8):
                entry = columns[u][k][t : t + 1, :]
                for i in live:
                    columns[u][i] = columns[u][i] - factors[i] * entry
            pivot_row = blocks[k][t : t + 1, :]
            for i in live:
                blocks[i] = blocks[i] - factors[i] * pivot_row
        done.append(blocks[k] * jnp.sqrt(scale))
    return jnp.concatenate(done, axis=0)[:, :n]


def exact_dot(a, b):
    return lax.dot_general(
        a, b, (((1,), (0,)), ((), ())), precision=lax.Precision.HIGHEST, preferred_element_type=F32
    )


def gram_of_parts(parts_ref, start, rank):
    parts = [parts_ref[i, :, start : start + 2 * rank].astype(F32) for i in range(parts_ref.shape[0])]
    summed = parts[0]
    for part in parts[1:]:
        summed = summed + part
    return summed[:, :rank] + summed[:, rank:]


def inverse_of(arrived, start):
    rank = arrived.shape[1]

    def kernel(arrived_ref, out_ref):
        out_ref[...] = inverse_factor(gram_of_parts(arrived_ref, start, rank))

    return pl.pallas_call(
        kernel,
        in_specs=[WHOLE],
        out_specs=WHOLE,
        out_shape=pltpu.VMEM((rank, rank), F32),
        cost_estimate=pl.CostEstimate(flops=60_000_000, bytes_accessed=200_000, transcendentals=0),
        name="inverse_of",
    )(on_chip(arrived))


def normalized_weighted(arrived, inverse, slope):
    count, rank, width = arrived.shape

    def kernel(arrived_ref, inverse_ref, slope_ref, out_ref):
        summed = arrived_ref[0].astype(F32)
        for i in range(1, count):
            summed = summed + arrived_ref[i].astype(F32)
        forward = (slope_ref[...] * exact_dot(inverse_ref[...], summed)).astype(BF16)
        out_ref[...] = (slope_ref[...] * forward.astype(F32)).astype(BF16)

    return pl.pallas_call(
        kernel,
        in_specs=[WHOLE] * 3,
        out_specs=WHOLE,
        out_shape=pltpu.VMEM((rank, width), BF16),
        name="normalized_weighted",
    )(on_chip(arrived), on_chip(inverse), on_chip(slope))


def normalized_panels(core, inverse, inverse_there, image, there):
    rank, width = there.shape

    def kernel(core_ref, inverse_ref, inverse_there_ref, image_ref, there_ref, out_ref):
        here_at = core_ref[0]
        here = exact_dot(inverse_ref[...], image_ref[:, :width].astype(F32))
        out_ref[pl.ds(here_at, 1)] = here[None]
        away = exact_dot(inverse_there_ref[...], there_ref[...].astype(F32))
        out_ref[pl.ds(1 - here_at, 1)] = away[None]

    return pl.pallas_call(
        kernel,
        in_specs=[pl.BlockSpec(memory_space=pltpu.SMEM)] + [WHOLE] * 4,
        out_specs=WHOLE,
        out_shape=jax.ShapeDtypeStruct((2, rank, width), F32),
        name="normalized_panels",
    )(core, on_chip(inverse), on_chip(inverse_there), on_chip(image), on_chip(there))


def three_parts(x):
    high = lax.reduce_precision(x, 8, 7)
    middle = lax.reduce_precision(x - high, 8, 7)
    return high.astype(BF16), middle.astype(BF16), (x - high - middle).astype(BF16)


def high_low(gram):
    high = lax.reduce_precision(gram, 8, 7)
    return jnp.concatenate([high.astype(BF16), (gram - high).astype(BF16)], axis=1)


def make(n_x, n_y, n_z):
    turns = [
        [(i * n_x + j, j * n_x + (i + turn) % n_x) for i in range(n_y) for j in range(n_x)]
        for turn in range(n_x)
    ]
    flip = [(0, 1), (1, 0)]

    def on_device(weights, preact, panel):
        core = lax.axis_index("core")
        first = core == 0
        _, rank, width_in = panel.shape
        width_row = weights.shape[1]
        w1_own, w2_own = weights[0], weights[1]

        partial_out = jnp.einsum("bki,oi->bko", panel, w1_own, preferred_element_type=F32)
        mine = jnp.where(first, partial_out[0], partial_out[1])
        theirs = jnp.where(first, partial_out[1], partial_out[0])
        summed_out = mine + lax.ppermute(theirs, "core", flip)

        slopes = 1.0 - jnp.tanh(jnp.where(first, preact[0], preact[1])) ** 2
        slope_1 = slopes[0:1]

        cut = width_row // n_x
        high, middle, low = three_parts(slopes[1:2])
        pad = jnp.zeros((8 - 3, width_in), BF16)
        extra = jnp.concatenate([jnp.pad(p, ((0, 0), (0, width_in - width_row))) for p in (high, middle, low)] + [pad])
        y_at, x_at = lax.axis_index("y"), lax.axis_index("x")
        moved = []
        for turn in range(n_x):
            start = lax.rem(y_at + turn, n_x) * cut
            piece = lax.dynamic_slice(w2_own, (start, 0), (cut, width_in), allow_negative_indices=False)
            moved.append(lax.ppermute(jnp.concatenate([piece, extra]), ("y", "x"), turns[turn]))
        here = jnp.concatenate([block[:cut] for block in moved])
        sent = jnp.concatenate([block[cut : cut + 3].astype(F32).sum(0, keepdims=True)[:, :width_row] for block in moved])
        slope_2 = lax.dynamic_slice(sent, (0, x_at * cut), (n_x, cut), allow_negative_indices=False).reshape(1, width_row)
        there = lax.ppermute(here, "core", flip)
        w2 = jnp.concatenate([jnp.where(first, here, there), jnp.where(first, there, here)], axis=1)
        w2, slope_2 = lax.optimization_barrier((w2, slope_2))
        w1_other = lax.ppermute(w1_own, "core", flip)

        image = inverse = None
        for iteration in range(ITERS):
            if iteration == 0:
                arrived = to_all(summed_out.astype(BF16), "x", n_x)
            else:
                own, other = image[:, :width_in], image[:, width_in:]
                partial_out = dot_t(own, w1_own) + dot_t(other, w1_other)
                gram = dot_t(own, own) + dot_t(other, other)
                message = jnp.concatenate([partial_out.astype(BF16), high_low(gram)], axis=1)
                arrived = to_all(message, "x", n_x)
                inverse = inverse_of(arrived, width_row)
            forward = (slope_1 * total(arrived[:, :, :width_row])).astype(BF16)
            spread = to_all(forward, "z", n_z)
            spread = jnp.moveaxis(spread, 0, 1).reshape(rank, n_z * width_row)
            partial_out = dot_t(spread, w2)
            arrived = to_all(partial_out.astype(BF16), "y", n_y)
            if inverse is None:
                forward = (slope_2 * total(arrived)).astype(BF16)
                weighted = (slope_2 * forward.astype(F32)).astype(BF16)
            else:
                weighted = normalized_weighted(arrived, inverse, slope_2)
            partial_in = dot_n(weighted, w2).astype(BF16)
            blocks = jnp.moveaxis(partial_in.reshape(rank, n_z, width_row), 1, 0)
            summed = total(exchange(blocks, "z")).astype(BF16)
            cotangent = total(to_all(summed, "x", n_x)).astype(BF16)
            weighted = (slope_1 * cotangent.astype(F32)).astype(BF16)
            partial_in = jnp.concatenate([dot_n(weighted, w1_own), dot_n(weighted, w1_other)], axis=1)
            groups = rank // 8
            cuts = n_y * n_z // groups
            length = 2 * width_in // cuts
            pieces = partial_in.astype(BF16).reshape(groups, 8, cuts, length)
            pieces = jnp.moveaxis(pieces, 2, 1).reshape(groups * cuts, 8, length)
            piece = total(exchange(pieces, ("y", "z"))).astype(BF16)
            image = to_all(piece, ("y", "z"), groups * cuts).reshape(groups, cuts, 8, length)
            image = jnp.moveaxis(image, 1, 2).reshape(rank, 2 * width_in)
        there = lax.ppermute(image[:, width_in:], "core", flip)
        gram = dot_t(image, image)
        inverse = inverse_of(to_all(high_low(gram), "x", n_x), 0)
        inverse_there = lax.ppermute(inverse, "core", flip)
        return normalized_panels(core.reshape(1).astype(jnp.int32), inverse, inverse_there, image, there)

    return on_device


def solution(mesh):
    n_x, n_y, n_z = 4, 4, 8
    fine = Mesh(mesh.devices.reshape(n_y, n_z, n_x, 2), ("y", "z", "x", "core"))
    on_device = make(n_x, n_y, n_z)

    return jax.shard_map(
        on_device,
        mesh=fine,
        in_specs=(P(None, ("y", "z"), ("x", "core")), P(None, None, ("y", "z")), P(None, None, ("x", "core"))),
        out_specs=P(None, None, ("x", "core")),
        check_vma=False,
    )
```

```python
import jax
import jax.numpy as jnp
from jax import lax
from jax.experimental import pallas as pl
from jax.experimental.pallas import tpu as pltpu
from jax.sharding import Mesh, PartitionSpec as P


WIDTH = 8192
ITERS = 2
BF16 = jnp.bfloat16
F32 = jnp.float32
WHOLE = pl.BlockSpec(memory_space=pltpu.VMEM)


def on_chip(x):
    return pltpu.with_memory_space_constraint(x, pltpu.VMEM)


def dot_t(a, w):
    return lax.dot_general(a, w, (((1,), (1,)), ((), ())), preferred_element_type=F32)


def dot_n(a, w):
    return lax.dot_general(a, w, (((1,), (0,)), ((), ())), preferred_element_type=F32)


def exchange(tiles, axis):
    return lax.all_to_all(tiles, axis, split_axis=0, concat_axis=0, tiled=True)


def to_all(x, axis, count):
    return exchange(jnp.broadcast_to(x[None], (count, *x.shape)), axis)


def total(tiles):
    return jnp.sum(tiles.astype(F32), axis=0)


def inverse_factor(gram):
    n = gram.shape[0]
    count = n // 8
    rows = lax.broadcasted_iota(jnp.int32, (n, n), 0)
    cols = lax.broadcasted_iota(jnp.int32, (n, n), 1)
    both = jnp.concatenate([(rows == cols).astype(F32), gram * (1.0 / WIDTH)], axis=1)
    blocks = [both[8 * i : 8 * i + 8] for i in range(count)]
    row_of = lax.broadcasted_iota(jnp.int32, (8, 2 * n), 0)
    done = []
    for k in range(count):
        live = range(k, count)
        columns = [
            {i: jnp.broadcast_to(blocks[i][:, n + 8 * k + t : n + 8 * k + t + 1], (8, 2 * n)) for i in live}
            for t in range(8)
        ]
        scale = jnp.zeros((8, 2 * n), F32)
        for t in range(8):
            inverse = 1.0 / columns[t][k][t : t + 1, :]
            scale = jnp.where(row_of == t, inverse, scale)
            factors = {i: columns[t][i] * inverse for i in live}
            factors[k] = jnp.where(row_of > t, factors[k], 0.0)
            for u in range(t + 1, 8):
                entry = columns[u][k][t : t + 1, :]
                for i in live:
                    columns[u][i] = columns[u][i] - factors[i] * entry
            pivot_row = blocks[k][t : t + 1, :]
            for i in live:
                blocks[i] = blocks[i] - factors[i] * pivot_row
        done.append(blocks[k] * jnp.sqrt(scale))
    return jnp.concatenate(done, axis=0)[:, :n]


def exact_dot(a, b):
    return lax.dot_general(
        a, b, (((1,), (0,)), ((), ())), precision=lax.Precision.HIGHEST, preferred_element_type=F32
    )


def gram_of_parts(parts_ref, start, rank):
    parts = [parts_ref[i, :, start : start + 2 * rank].astype(F32) for i in range(parts_ref.shape[0])]
    summed = parts[0]
    for part in parts[1:]:
        summed = summed + part
    return summed[:, :rank] + summed[:, rank:]


def inverse_of(arrived, start):
    rank = arrived.shape[1]

    def kernel(arrived_ref, out_ref):
        out_ref[...] = inverse_factor(gram_of_parts(arrived_ref, start, rank))

    return pl.pallas_call(
        kernel,
        in_specs=[WHOLE],
        out_specs=WHOLE,
        out_shape=pltpu.VMEM((rank, rank), F32),
        cost_estimate=pl.CostEstimate(flops=60_000_000, bytes_accessed=200_000, transcendentals=0),
        name="inverse_of",
    )(on_chip(arrived))


def normalized_forward(arrived, slope, width):
    count, rank, _ = arrived.shape

    def kernel(arrived_ref, slope_ref, out_ref):
        inverse = inverse_factor(gram_of_parts(arrived_ref, width, rank))
        summed = arrived_ref[0, :, :width].astype(F32)
        for i in range(1, count):
            summed = summed + arrived_ref[i, :, :width].astype(F32)
        out_ref[...] = (slope_ref[...] * exact_dot(inverse, summed)).astype(BF16)

    return pl.pallas_call(
        kernel,
        in_specs=[WHOLE] * 2,
        out_specs=WHOLE,
        out_shape=pltpu.VMEM((rank, width), BF16),
        name="normalized_forward",
    )(on_chip(arrived), on_chip(slope))


def normalized_panels(core, inverse, inverse_there, image, there):
    rank, width = there.shape

    def kernel(core_ref, inverse_ref, inverse_there_ref, image_ref, there_ref, out_ref):
        here_at = core_ref[0]
        here = exact_dot(inverse_ref[...], image_ref[:, :width].astype(F32))
        out_ref[pl.ds(here_at, 1)] = here[None]
        away = exact_dot(inverse_there_ref[...], there_ref[...].astype(F32))
        out_ref[pl.ds(1 - here_at, 1)] = away[None]

    return pl.pallas_call(
        kernel,
        in_specs=[pl.BlockSpec(memory_space=pltpu.SMEM)] + [WHOLE] * 4,
        out_specs=WHOLE,
        out_shape=jax.ShapeDtypeStruct((2, rank, width), F32),
        name="normalized_panels",
    )(core, on_chip(inverse), on_chip(inverse_there), on_chip(image), on_chip(there))


def three_parts(x):
    high = lax.reduce_precision(x, 8, 7)
    middle = lax.reduce_precision(x - high, 8, 7)
    return high.astype(BF16), middle.astype(BF16), (x - high - middle).astype(BF16)


def high_low(gram):
    high = lax.reduce_precision(gram, 8, 7)
    return jnp.concatenate([high.astype(BF16), (gram - high).astype(BF16)], axis=1)


def make(n_x, n_y, n_z):
    turns = [
        [(i * n_x + j, j * n_x + (i + turn) % n_x) for i in range(n_y) for j in range(n_x)]
        for turn in range(n_x)
    ]
    flip = [(0, 1), (1, 0)]

    def on_device(weights, preact, panel):
        core = lax.axis_index("core")
        first = core == 0
        _, rank, width_in = panel.shape
        width_row = weights.shape[1]
        w1_own, w2_own = weights[0], weights[1]

        partial_out = jnp.einsum("bki,oi->bko", panel, w1_own, preferred_element_type=F32)
        mine = jnp.where(first, partial_out[0], partial_out[1])
        theirs = jnp.where(first, partial_out[1], partial_out[0])
        summed_out = mine + lax.ppermute(theirs, "core", flip)

        slopes = 1.0 - jnp.tanh(jnp.where(first, preact[0], preact[1])) ** 2
        slope_1 = slopes[0:1]

        cut = width_row // n_x
        high, middle, low = three_parts(slopes[1:2])
        pad = jnp.zeros((8 - 3, width_in), BF16)
        extra = jnp.concatenate([jnp.pad(p, ((0, 0), (0, width_in - width_row))) for p in (high, middle, low)] + [pad])
        y_at, x_at = lax.axis_index("y"), lax.axis_index("x")
        moved = []
        for turn in range(n_x):
            start = lax.rem(y_at + turn, n_x) * cut
            piece = lax.dynamic_slice(w2_own, (start, 0), (cut, width_in), allow_negative_indices=False)
            moved.append(lax.ppermute(jnp.concatenate([piece, extra]), ("y", "x"), turns[turn]))
        here = jnp.concatenate([block[:cut] for block in moved])
        sent = jnp.concatenate([block[cut : cut + 3].astype(F32).sum(0, keepdims=True)[:, :width_row] for block in moved])
        slope_2 = lax.dynamic_slice(sent, (0, x_at * cut), (n_x, cut), allow_negative_indices=False).reshape(1, width_row)
        there = lax.ppermute(here, "core", flip)
        w2 = jnp.concatenate([jnp.where(first, here, there), jnp.where(first, there, here)], axis=1)
        w1_other = lax.ppermute(w1_own, "core", flip)
        w2, slope_2, w1_other = lax.optimization_barrier((w2, slope_2, w1_other))

        image = None
        for iteration in range(ITERS):
            if iteration == 0:
                arrived = to_all(summed_out.astype(BF16), "x", n_x)
                forward = (slope_1 * total(arrived)).astype(BF16)
            else:
                own, other = image[:, :width_in], image[:, width_in:]
                partial_out = dot_t(own, w1_own) + dot_t(other, w1_other)
                gram = dot_t(own, own) + dot_t(other, other)
                message = jnp.concatenate([partial_out.astype(BF16), high_low(gram)], axis=1)
                arrived = to_all(message, "x", n_x)
                forward = normalized_forward(arrived, slope_1, width_row)
            spread = to_all(forward, "z", n_z)
            spread = jnp.moveaxis(spread, 0, 1).reshape(rank, n_z * width_row)
            partial_out = dot_t(spread, w2)
            arrived = to_all(partial_out.astype(BF16), "y", n_y)
            forward = (slope_2 * total(arrived)).astype(BF16)
            weighted = (slope_2 * forward.astype(F32)).astype(BF16)
            partial_in = dot_n(weighted, w2).astype(BF16)
            blocks = jnp.moveaxis(partial_in.reshape(rank, n_z, width_row), 1, 0)
            summed = total(exchange(blocks, "z")).astype(BF16)
            cotangent = total(to_all(summed, "x", n_x)).astype(BF16)
            weighted = (slope_1 * cotangent.astype(F32)).astype(BF16)
            partial_in = jnp.concatenate([dot_n(weighted, w1_own), dot_n(weighted, w1_other)], axis=1)
            groups = rank // 8
            cuts = n_y * n_z // groups
            length = 2 * width_in // cuts
            pieces = partial_in.astype(BF16).reshape(groups, 8, cuts, length)
            pieces = jnp.moveaxis(pieces, 2, 1).reshape(groups * cuts, 8, length)
            piece = total(exchange(pieces, ("y", "z"))).astype(BF16)
            image = to_all(piece, ("y", "z"), groups * cuts).reshape(groups, cuts, 8, length)
            image = jnp.moveaxis(image, 1, 2).reshape(rank, 2 * width_in)
        there = lax.ppermute(image[:, width_in:], "core", flip)
        gram = dot_t(image, image)
        inverse = inverse_of(to_all(high_low(gram), "x", n_x), 0)
        inverse_there = lax.ppermute(inverse, "core", flip)
        return normalized_panels(core.reshape(1).astype(jnp.int32), inverse, inverse_there, image, there)

    return on_device


def solution(mesh):
    n_x, n_y, n_z = 4, 4, 8
    fine = Mesh(mesh.devices.reshape(n_y, n_z, n_x, 2), ("y", "z", "x", "core"))
    on_device = make(n_x, n_y, n_z)

    return jax.shard_map(
        on_device,
        mesh=fine,
        in_specs=(P(None, ("y", "z"), ("x", "core")), P(None, None, ("y", "z")), P(None, None, ("x", "core"))),
        out_specs=P(None, None, ("x", "core")),
        check_vma=False,
    )
```

```python
import jax
import jax.numpy as jnp
from jax import lax
from jax.experimental import pallas as pl
from jax.experimental.pallas import tpu as pltpu
from jax.sharding import Mesh, PartitionSpec as P


WIDTH = 8192
ITERS = 2
BF16 = jnp.bfloat16
F32 = jnp.float32
WHOLE = pl.BlockSpec(memory_space=pltpu.VMEM)


def on_chip(x):
    return pltpu.with_memory_space_constraint(x, pltpu.VMEM)


def dot_t(a, w):
    return lax.dot_general(a, w, (((1,), (1,)), ((), ())), preferred_element_type=F32)


def dot_n(a, w):
    return lax.dot_general(a, w, (((1,), (0,)), ((), ())), preferred_element_type=F32)


def exchange(tiles, axis):
    return lax.all_to_all(tiles, axis, split_axis=0, concat_axis=0, tiled=True)


def to_all(x, axis, count):
    return exchange(jnp.broadcast_to(x[None], (count, *x.shape)), axis)


def total(tiles):
    return jnp.sum(tiles.astype(F32), axis=0)


def inverse_factor(gram):
    n = gram.shape[0]
    count = n // 8
    rows = lax.broadcasted_iota(jnp.int32, (n, n), 0)
    cols = lax.broadcasted_iota(jnp.int32, (n, n), 1)
    both = jnp.concatenate([(rows == cols).astype(F32), gram * (1.0 / WIDTH)], axis=1)
    blocks = [both[8 * i : 8 * i + 8] for i in range(count)]
    row_of = lax.broadcasted_iota(jnp.int32, (8, 2 * n), 0)
    done = []
    for k in range(count):
        live = range(k, count)
        columns = [
            {i: jnp.broadcast_to(blocks[i][:, n + 8 * k + t : n + 8 * k + t + 1], (8, 2 * n)) for i in live}
            for t in range(8)
        ]
        scale = jnp.zeros((8, 2 * n), F32)
        for t in range(8):
            inverse = 1.0 / columns[t][k][t : t + 1, :]
            scale = jnp.where(row_of == t, inverse, scale)
            factors = {i: columns[t][i] * inverse for i in live}
            factors[k] = jnp.where(row_of > t, factors[k], 0.0)
            for u in range(t + 1, 8):
                entry = columns[u][k][t : t + 1, :]
                for i in live:
                    columns[u][i] = columns[u][i] - factors[i] * entry
            pivot_row = blocks[k][t : t + 1, :]
            for i in live:
                blocks[i] = blocks[i] - factors[i] * pivot_row
        done.append(blocks[k] * jnp.sqrt(scale))
    return jnp.concatenate(done, axis=0)[:, :n]


def exact_dot(a, b):
    return lax.dot_general(
        a, b, (((1,), (0,)), ((), ())), precision=lax.Precision.HIGHEST, preferred_element_type=F32
    )


def gram_of_parts(parts_ref, start, rank):
    parts = [parts_ref[i, :, start : start + 2 * rank].astype(F32) for i in range(parts_ref.shape[0])]
    summed = parts[0]
    for part in parts[1:]:
        summed = summed + part
    return summed[:, :rank] + summed[:, rank:]


def inverse_of(arrived, start):
    rank = arrived.shape[1]

    def kernel(arrived_ref, out_ref):
        out_ref[...] = inverse_factor(gram_of_parts(arrived_ref, start, rank))

    return pl.pallas_call(
        kernel,
        in_specs=[WHOLE],
        out_specs=WHOLE,
        out_shape=pltpu.VMEM((rank, rank), F32),
        cost_estimate=pl.CostEstimate(flops=60_000_000, bytes_accessed=200_000, transcendentals=0),
        name="inverse_of",
    )(on_chip(arrived))


def normalized_forward(arrived, slope, width):
    count, rank, _ = arrived.shape

    def kernel(arrived_ref, slope_ref, out_ref):
        inverse = inverse_factor(gram_of_parts(arrived_ref, width, rank))
        summed = arrived_ref[0, :, :width].astype(F32)
        for i in range(1, count):
            summed = summed + arrived_ref[i, :, :width].astype(F32)
        out_ref[...] = (slope_ref[...] * exact_dot(inverse, summed)).astype(BF16)

    return pl.pallas_call(
        kernel,
        in_specs=[WHOLE] * 2,
        out_specs=WHOLE,
        out_shape=pltpu.VMEM((rank, width), BF16),
        name="normalized_forward",
    )(on_chip(arrived), on_chip(slope))


def normalized_panels(core, inverse, inverse_there, image, there):
    rank, width = there.shape

    def kernel(core_ref, inverse_ref, inverse_there_ref, image_ref, there_ref, out_ref):
        here_at = core_ref[0]
        here = exact_dot(inverse_ref[...], image_ref[:, :width].astype(F32))
        out_ref[pl.ds(here_at, 1)] = here[None]
        away = exact_dot(inverse_there_ref[...], there_ref[...].astype(F32))
        out_ref[pl.ds(1 - here_at, 1)] = away[None]

    return pl.pallas_call(
        kernel,
        in_specs=[pl.BlockSpec(memory_space=pltpu.SMEM)] + [WHOLE] * 4,
        out_specs=WHOLE,
        out_shape=jax.ShapeDtypeStruct((2, rank, width), F32),
        name="normalized_panels",
    )(core, on_chip(inverse), on_chip(inverse_there), on_chip(image), on_chip(there))


def three_parts(x):
    high = lax.reduce_precision(x, 8, 7)
    middle = lax.reduce_precision(x - high, 8, 7)
    return high.astype(BF16), middle.astype(BF16), (x - high - middle).astype(BF16)


def high_low(gram):
    high = lax.reduce_precision(gram, 8, 7)
    return jnp.concatenate([high.astype(BF16), (gram - high).astype(BF16)], axis=1)


def make(n_x, n_y, n_z):
    turns = [
        [(i * n_x + j, j * n_x + (i + turn) % n_x) for i in range(n_y) for j in range(n_x)]
        for turn in range(n_x)
    ]
    flip = [(0, 1), (1, 0)]

    def on_device(weights, preact, panel):
        core = lax.axis_index("core")
        first = core == 0
        _, rank, width_in = panel.shape
        width_row = weights.shape[1]
        w1_own, w2_own = weights[0], weights[1]

        partial_out = jnp.einsum("bki,oi->bko", panel, w1_own, preferred_element_type=F32)
        mine = jnp.where(first, partial_out[0], partial_out[1])
        theirs = jnp.where(first, partial_out[1], partial_out[0])
        summed_out = mine + lax.ppermute(theirs, "core", flip)

        slopes = 1.0 - jnp.tanh(jnp.where(first, preact[0], preact[1])) ** 2
        slope_1 = slopes[0:1]

        cut = width_row // n_x
        y_at, x_at = lax.axis_index("y"), lax.axis_index("x")
        slope_piece = lax.dynamic_slice(slopes[1:2], (0, x_at * cut), (1, cut), allow_negative_indices=False)
        spot = lax.rem(x_at - y_at + n_x, n_x)
        at_turn = lax.broadcasted_iota(jnp.int32, (1, n_x, cut), 1) == spot
        slope_spread = jnp.where(at_turn, slope_piece[:, None], 0.0).reshape(1, width_row)
        slope_rows = jnp.concatenate([*three_parts(slope_spread), jnp.zeros((8 - 3, width_row), BF16)])

        blocks = []
        for turn in range(n_x):
            start = lax.rem(y_at + turn, n_x) * cut
            piece = lax.dynamic_slice(w2_own, (start, 0), (cut, width_in), allow_negative_indices=False)
            here = lax.ppermute(piece, ("y", "x"), turns[turn])
            there = lax.ppermute(here, "core", flip)
            blocks.append(jnp.concatenate([jnp.where(first, here, there), jnp.where(first, there, here)], axis=1))
        w1_other = lax.ppermute(w1_own, "core", flip)
        w2, w1_other = lax.optimization_barrier((jnp.concatenate(blocks), w1_other))

        image = None
        for iteration in range(ITERS):
            if iteration == 0:
                arrived = to_all(summed_out.astype(BF16), "x", n_x)
                forward = (slope_1 * total(arrived)).astype(BF16)
            else:
                own, other = image[:, :width_in], image[:, width_in:]
                partial_out = dot_t(own, w1_own) + dot_t(other, w1_other)
                gram = dot_t(own, own) + dot_t(other, other)
                message = jnp.concatenate([partial_out.astype(BF16), high_low(gram)], axis=1)
                arrived = to_all(message, "x", n_x)
                forward = normalized_forward(arrived, slope_1, width_row)
            spread = to_all(forward, "z", n_z)
            spread = jnp.moveaxis(spread, 0, 1).reshape(rank, n_z * width_row)
            partial_out = dot_t(spread, w2).astype(BF16)
            if iteration == 0:
                arrived = to_all(jnp.concatenate([partial_out, slope_rows]), "y", n_y)
                slope_2 = total(arrived[:, rank:]).sum(axis=0, keepdims=True)
                arrived = arrived[:, :rank]
            else:
                arrived = to_all(partial_out, "y", n_y)
            forward = (slope_2 * total(arrived)).astype(BF16)
            weighted = (slope_2 * forward.astype(F32)).astype(BF16)
            partial_in = dot_n(weighted, w2).astype(BF16)
            blocks = jnp.moveaxis(partial_in.reshape(rank, n_z, width_row), 1, 0)
            summed = total(exchange(blocks, "z")).astype(BF16)
            cotangent = total(to_all(summed, "x", n_x)).astype(BF16)
            weighted = (slope_1 * cotangent.astype(F32)).astype(BF16)
            partial_in = jnp.concatenate([dot_n(weighted, w1_own), dot_n(weighted, w1_other)], axis=1)
            groups = rank // 8
            cuts = n_y * n_z // groups
            length = 2 * width_in // cuts
            pieces = partial_in.astype(BF16).reshape(groups, 8, cuts, length)
            pieces = jnp.moveaxis(pieces, 2, 1).reshape(groups * cuts, 8, length)
            piece = total(exchange(pieces, ("y", "z"))).astype(BF16)
            image = to_all(piece, ("y", "z"), groups * cuts).reshape(groups, cuts, 8, length)
            image = jnp.moveaxis(image, 1, 2).reshape(rank, 2 * width_in)
        there = lax.ppermute(image[:, width_in:], "core", flip)
        gram = dot_t(image, image)
        inverse = inverse_of(to_all(high_low(gram), "x", n_x), 0)
        inverse_there = lax.ppermute(inverse, "core", flip)
        return normalized_panels(core.reshape(1).astype(jnp.int32), inverse, inverse_there, image, there)

    return on_device


def solution(mesh):
    n_x, n_y, n_z = 4, 4, 8
    fine = Mesh(mesh.devices.reshape(n_y, n_z, n_x, 2), ("y", "z", "x", "core"))
    on_device = make(n_x, n_y, n_z)

    return jax.shard_map(
        on_device,
        mesh=fine,
        in_specs=(P(None, ("y", "z"), ("x", "core")), P(None, None, ("y", "z")), P(None, None, ("x", "core"))),
        out_specs=P(None, None, ("x", "core")),
        check_vma=False,
    )
```

```python
import jax
import jax.numpy as jnp
from jax import lax
from jax.experimental import pallas as pl
from jax.experimental.pallas import tpu as pltpu
from jax.sharding import Mesh, PartitionSpec as P


WIDTH = 8192
ITERS = 2
BF16 = jnp.bfloat16
F32 = jnp.float32
WHOLE = pl.BlockSpec(memory_space=pltpu.VMEM)


def on_chip(x):
    return pltpu.with_memory_space_constraint(x, pltpu.VMEM)


def dot_t(a, w):
    return lax.dot_general(a, w, (((1,), (1,)), ((), ())), preferred_element_type=F32)


def dot_n(a, w):
    return lax.dot_general(a, w, (((1,), (0,)), ((), ())), preferred_element_type=F32)


def exchange(tiles, axis):
    return lax.all_to_all(tiles, axis, split_axis=0, concat_axis=0, tiled=True)


def to_all(x, axis, count):
    return exchange(jnp.broadcast_to(x[None], (count, *x.shape)), axis)


def total(tiles):
    return jnp.sum(tiles.astype(F32), axis=0)


def inverse_factor(gram):
    n = gram.shape[0]
    count = n // 8
    rows = lax.broadcasted_iota(jnp.int32, (n, n), 0)
    cols = lax.broadcasted_iota(jnp.int32, (n, n), 1)
    both = jnp.concatenate([(rows == cols).astype(F32), gram * (1.0 / WIDTH)], axis=1)
    blocks = [both[8 * i : 8 * i + 8] for i in range(count)]
    row_of = lax.broadcasted_iota(jnp.int32, (8, 2 * n), 0)
    done = []
    for k in range(count):
        live = range(k, count)
        columns = [
            {i: jnp.broadcast_to(blocks[i][:, n + 8 * k + t : n + 8 * k + t + 1], (8, 2 * n)) for i in live}
            for t in range(8)
        ]
        scale = jnp.zeros((8, 2 * n), F32)
        for t in range(8):
            inverse = 1.0 / columns[t][k][t : t + 1, :]
            scale = jnp.where(row_of == t, inverse, scale)
            factors = {i: columns[t][i] * inverse for i in live}
            factors[k] = jnp.where(row_of > t, factors[k], 0.0)
            for u in range(t + 1, 8):
                entry = columns[u][k][t : t + 1, :]
                for i in live:
                    columns[u][i] = columns[u][i] - factors[i] * entry
            pivot_row = blocks[k][t : t + 1, :]
            for i in live:
                blocks[i] = blocks[i] - factors[i] * pivot_row
        done.append(blocks[k] * jnp.sqrt(scale))
    return jnp.concatenate(done, axis=0)[:, :n]


def exact_dot(a, b):
    return lax.dot_general(
        a, b, (((1,), (0,)), ((), ())), precision=lax.Precision.HIGHEST, preferred_element_type=F32
    )


def gram_of_parts(parts_ref, start, rank):
    parts = [parts_ref[i, :, start : start + 2 * rank].astype(F32) for i in range(parts_ref.shape[0])]
    summed = parts[0]
    for part in parts[1:]:
        summed = summed + part
    return summed[:, :rank] + summed[:, rank:]


def inverse_of(arrived, start):
    rank = arrived.shape[1]

    def kernel(arrived_ref, out_ref):
        out_ref[...] = inverse_factor(gram_of_parts(arrived_ref, start, rank))

    return pl.pallas_call(
        kernel,
        in_specs=[WHOLE],
        out_specs=WHOLE,
        out_shape=pltpu.VMEM((rank, rank), F32),
        cost_estimate=pl.CostEstimate(flops=60_000_000, bytes_accessed=200_000, transcendentals=0),
        name="inverse_of",
    )(on_chip(arrived))


def normalized_forward(arrived, slope, width):
    count, rank, _ = arrived.shape

    def kernel(arrived_ref, slope_ref, out_ref):
        inverse = inverse_factor(gram_of_parts(arrived_ref, width, rank))
        summed = arrived_ref[0, :, :width].astype(F32)
        for i in range(1, count):
            summed = summed + arrived_ref[i, :, :width].astype(F32)
        out_ref[...] = (slope_ref[...] * exact_dot(inverse, summed)).astype(BF16)

    return pl.pallas_call(
        kernel,
        in_specs=[WHOLE] * 2,
        out_specs=WHOLE,
        out_shape=pltpu.VMEM((rank, width), BF16),
        name="normalized_forward",
    )(on_chip(arrived), on_chip(slope))


def normalized_panels(core, inverse, inverse_there, image, there):
    rank, width = there.shape

    def kernel(core_ref, inverse_ref, inverse_there_ref, image_ref, there_ref, out_ref):
        here_at = core_ref[0]
        here = exact_dot(inverse_ref[...], image_ref[:, :width].astype(F32))
        out_ref[pl.ds(here_at, 1)] = here[None]
        away = exact_dot(inverse_there_ref[...], there_ref[...].astype(F32))
        out_ref[pl.ds(1 - here_at, 1)] = away[None]

    return pl.pallas_call(
        kernel,
        in_specs=[pl.BlockSpec(memory_space=pltpu.SMEM)] + [WHOLE] * 4,
        out_specs=WHOLE,
        out_shape=jax.ShapeDtypeStruct((2, rank, width), F32),
        name="normalized_panels",
    )(core, on_chip(inverse), on_chip(inverse_there), on_chip(image), on_chip(there))


def three_parts(x):
    high = lax.reduce_precision(x, 8, 7)
    middle = lax.reduce_precision(x - high, 8, 7)
    return high.astype(BF16), middle.astype(BF16), (x - high - middle).astype(BF16)


def high_low(gram):
    high = lax.reduce_precision(gram, 8, 7)
    return jnp.concatenate([high.astype(BF16), (gram - high).astype(BF16)], axis=1)


def make(n_x, n_y, n_z):
    share = n_x // 2
    turns = [
        [
            ((i * n_x + j) * 2 + c, (j * n_x + (i + share * c + e) % n_x) * 2 + c)
            for i in range(n_y)
            for j in range(n_x)
            for c in range(2)
        ]
        for e in range(share)
    ]
    flip = [(0, 1), (1, 0)]

    def on_device(weights, preact, panel):
        core = lax.axis_index("core")
        first = core == 0
        _, rank, width_in = panel.shape
        width_row = weights.shape[1]
        w1_own, w2_own = weights[0], weights[1]

        partial_out = jnp.einsum("bki,oi->bko", panel, w1_own, preferred_element_type=F32)
        mine = jnp.where(first, partial_out[0], partial_out[1])
        theirs = jnp.where(first, partial_out[1], partial_out[0])
        traded = lax.ppermute(theirs, "core", flip)
        summed_out = mine + traded

        slopes = 1.0 - jnp.tanh(jnp.where(first, preact[0], preact[1])) ** 2
        slope_1 = slopes[0:1]

        cut = width_row // n_x
        y_at, x_at = lax.axis_index("y"), lax.axis_index("x")
        slope_piece = lax.dynamic_slice(slopes[1:2], (0, x_at * cut), (1, cut), allow_negative_indices=False)
        spot = lax.rem(x_at - y_at + n_x, n_x)
        at_turn = lax.broadcasted_iota(jnp.int32, (1, n_x, cut), 1) == spot
        slope_spread = jnp.where(at_turn, slope_piece[:, None], 0.0).reshape(1, width_row)
        slope_rows = jnp.concatenate([*three_parts(slope_spread), jnp.zeros((8 - 3, width_row), BF16)])

        def piece(turn):
            start = lax.rem(y_at + turn, n_x) * cut
            return lax.dynamic_slice(w2_own, (start, 0), (cut, width_in), allow_negative_indices=False)

        kept = jnp.concatenate([piece(core * share + e) for e in range(share)])
        got = lax.ppermute(jnp.concatenate([piece((1 - core) * share + e) for e in range(share)]), "core", flip)
        rows = jnp.concatenate([jnp.where(first, kept, got), jnp.where(first, got, kept)], axis=1)
        rows = [rows[e * cut : (e + 1) * cut] for e in range(share)]
        here = []
        for e in range(share):
            here.append(lax.ppermute(rows[e], ("y", "x", "core"), turns[e]))
        there = [lax.ppermute(block, "core", flip) for block in here]
        blocks = [jnp.where(first, h, t) for h, t in zip(here, there)]
        blocks += [jnp.where(first, t, h) for h, t in zip(here, there)]
        w1_other = lax.ppermute(w1_own, "core", flip)
        w2, w1_other = lax.optimization_barrier((jnp.concatenate(blocks), w1_other))

        image = None
        for iteration in range(ITERS):
            if iteration == 0:
                arrived = to_all(summed_out.astype(BF16), "x", n_x)
                forward = (slope_1 * total(arrived)).astype(BF16)
            else:
                own, other = image[:, :width_in], image[:, width_in:]
                partial_out = dot_t(own, w1_own) + dot_t(other, w1_other)
                gram = dot_t(own, own) + dot_t(other, other)
                message = jnp.concatenate([partial_out.astype(BF16), high_low(gram)], axis=1)
                arrived = to_all(message, "x", n_x)
                forward = normalized_forward(arrived, slope_1, width_row)
            spread = to_all(forward, "z", n_z)
            spread = jnp.moveaxis(spread, 0, 1).reshape(rank, n_z * width_row)
            partial_out = dot_t(spread, w2).astype(BF16)
            if iteration == 0:
                arrived = to_all(jnp.concatenate([partial_out, slope_rows]), "y", n_y)
                slope_2 = total(arrived[:, rank:]).sum(axis=0, keepdims=True)
                arrived = arrived[:, :rank]
            else:
                arrived = to_all(partial_out, "y", n_y)
            forward = (slope_2 * total(arrived)).astype(BF16)
            weighted = (slope_2 * forward.astype(F32)).astype(BF16)
            partial_in = dot_n(weighted, w2).astype(BF16)
            blocks = jnp.moveaxis(partial_in.reshape(rank, n_z, width_row), 1, 0)
            summed = total(exchange(blocks, "z")).astype(BF16)
            cotangent = total(to_all(summed, "x", n_x)).astype(BF16)
            weighted = (slope_1 * cotangent.astype(F32)).astype(BF16)
            partial_in = jnp.concatenate([dot_n(weighted, w1_own), dot_n(weighted, w1_other)], axis=1)
            groups = rank // 8
            cuts = n_y * n_z // groups
            length = 2 * width_in // cuts
            pieces = partial_in.astype(BF16).reshape(groups, 8, cuts, length)
            pieces = jnp.moveaxis(pieces, 2, 1).reshape(groups * cuts, 8, length)
            piece = total(exchange(pieces, ("y", "z"))).astype(BF16)
            image = to_all(piece, ("y", "z"), groups * cuts).reshape(groups, cuts, 8, length)
            image = jnp.moveaxis(image, 1, 2).reshape(rank, 2 * width_in)
        there = lax.ppermute(image[:, width_in:], "core", flip)
        gram = dot_t(image, image)
        inverse = inverse_of(to_all(high_low(gram), "x", n_x), 0)
        inverse_there = lax.ppermute(inverse, "core", flip)
        return normalized_panels(core.reshape(1).astype(jnp.int32), inverse, inverse_there, image, there)

    return on_device


def solution(mesh):
    n_x, n_y, n_z = 4, 4, 8
    fine = Mesh(mesh.devices.reshape(n_y, n_z, n_x, 2), ("y", "z", "x", "core"))
    on_device = make(n_x, n_y, n_z)

    return jax.shard_map(
        on_device,
        mesh=fine,
        in_specs=(P(None, ("y", "z"), ("x", "core")), P(None, None, ("y", "z")), P(None, None, ("x", "core"))),
        out_specs=P(None, None, ("x", "core")),
        check_vma=False,
    )
```

```python
import jax
import jax.numpy as jnp
from jax import lax
from jax.experimental import pallas as pl
from jax.experimental.pallas import tpu as pltpu
from jax.sharding import Mesh, PartitionSpec as P


WIDTH = 8192
ITERS = 2
BF16 = jnp.bfloat16
F32 = jnp.float32
WHOLE = pl.BlockSpec(memory_space=pltpu.VMEM)


def on_chip(x):
    return pltpu.with_memory_space_constraint(x, pltpu.VMEM)


def dot_t(a, w):
    return lax.dot_general(a, w, (((1,), (1,)), ((), ())), preferred_element_type=F32)


def dot_n(a, w):
    return lax.dot_general(a, w, (((1,), (0,)), ((), ())), preferred_element_type=F32)


def exchange(tiles, axis):
    return lax.all_to_all(tiles, axis, split_axis=0, concat_axis=0, tiled=True)


def to_all(x, axis, count):
    return exchange(jnp.broadcast_to(x[None], (count, *x.shape)), axis)


def total(tiles):
    return jnp.sum(tiles.astype(F32), axis=0)


def inverse_factors(grams):
    n = grams[0].shape[0]
    count = n // 8
    rows = lax.broadcasted_iota(jnp.int32, (n, n), 0)
    cols = lax.broadcasted_iota(jnp.int32, (n, n), 1)
    eye = (rows == cols).astype(F32)
    row_of = lax.broadcasted_iota(jnp.int32, (8, 2 * n), 0)
    many = []
    for gram in grams:
        both = jnp.concatenate([eye, gram * (1.0 / WIDTH)], axis=1)
        many.append([both[8 * i : 8 * i + 8] for i in range(count)])

    def columns_of(blocks, k):
        return [
            {i: jnp.broadcast_to(blocks[i][:, n + 8 * k + t : n + 8 * k + t + 1], (8, 2 * n)) for i in range(k, count)}
            for t in range(8)
        ]

    def step(blocks, columns, scale, k, t):
        live = range(k, count)
        inverse = 1.0 / columns[t][k][t : t + 1, :]
        factors = {i: columns[t][i] * inverse for i in live}
        factors[k] = jnp.where(row_of > t, factors[k], 0.0)
        for u in range(t + 1, 8):
            entry = columns[u][k][t : t + 1, :]
            for i in live:
                columns[u][i] = columns[u][i] - factors[i] * entry
        pivot_row = blocks[k][t : t + 1, :]
        for i in live:
            blocks[i] = blocks[i] - factors[i] * pivot_row
        return jnp.where(row_of == t, inverse, scale)

    done = [[] for _ in many]
    for k in range(count):
        columns = [columns_of(blocks, k) for blocks in many]
        scales = [jnp.zeros((8, 2 * n), F32) for _ in many]
        for t in range(8):
            for g, blocks in enumerate(many):
                scales[g] = step(blocks, columns[g], scales[g], k, t)
        for g, blocks in enumerate(many):
            done[g].append(blocks[k] * jnp.sqrt(scales[g]))
    return [jnp.concatenate(d, axis=0)[:, :n] for d in done]


def exact_dot(a, b):
    return lax.dot_general(
        a, b, (((1,), (0,)), ((), ())), precision=lax.Precision.HIGHEST, preferred_element_type=F32
    )


def gram_of_parts(parts_ref, start, rank):
    parts = [parts_ref[i, :, start : start + 2 * rank].astype(F32) for i in range(parts_ref.shape[0])]
    summed = parts[0]
    for part in parts[1:]:
        summed = summed + part
    return summed[:, :rank] + summed[:, rank:]


def normalized_forward(arrived, slope, width):
    count, rank, _ = arrived.shape

    def kernel(arrived_ref, slope_ref, out_ref):
        (inverse,) = inverse_factors([gram_of_parts(arrived_ref, width, rank)])
        summed = arrived_ref[0, :, :width].astype(F32)
        for i in range(1, count):
            summed = summed + arrived_ref[i, :, :width].astype(F32)
        out_ref[...] = (slope_ref[...] * exact_dot(inverse, summed)).astype(BF16)

    return pl.pallas_call(
        kernel,
        in_specs=[WHOLE] * 2,
        out_specs=WHOLE,
        out_shape=pltpu.VMEM((rank, width), BF16),
        name="normalized_forward",
    )(on_chip(arrived), on_chip(slope))


def normalized_panels(core, arrived, image, there):
    rank, width = there.shape

    def kernel(core_ref, arrived_ref, image_ref, there_ref, out_ref):
        here_at = core_ref[0]
        inverses = []
        for b in (here_at, 1 - here_at):
            gram = arrived_ref[pl.ds(b, 1)][0].astype(F32)
            for i in range(2, arrived_ref.shape[0], 2):
                gram = gram + arrived_ref[pl.ds(i + b, 1)][0].astype(F32)
            inverses.append(gram[:, :rank] + gram[:, rank:])
        inverses = inverse_factors(inverses)
        here = exact_dot(inverses[0], image_ref[:, :width].astype(F32))
        out_ref[pl.ds(here_at, 1)] = here[None]
        away = exact_dot(inverses[1], there_ref[...].astype(F32))
        out_ref[pl.ds(1 - here_at, 1)] = away[None]

    return pl.pallas_call(
        kernel,
        in_specs=[pl.BlockSpec(memory_space=pltpu.SMEM)] + [WHOLE] * 3,
        out_specs=WHOLE,
        out_shape=jax.ShapeDtypeStruct((2, rank, width), F32),
        name="normalized_panels",
    )(core, on_chip(arrived), on_chip(image), on_chip(there))


def three_parts(x):
    high = lax.reduce_precision(x, 8, 7)
    middle = lax.reduce_precision(x - high, 8, 7)
    return high.astype(BF16), middle.astype(BF16), (x - high - middle).astype(BF16)


def high_low(gram):
    high = lax.reduce_precision(gram, 8, 7)
    return jnp.concatenate([high.astype(BF16), (gram - high).astype(BF16)], axis=1)


def make(n_x, n_y, n_z):
    share = n_x // 2
    turns = [
        [
            ((i * n_x + j) * 2 + c, (j * n_x + (i + share * c + e) % n_x) * 2 + c)
            for i in range(n_y)
            for j in range(n_x)
            for c in range(2)
        ]
        for e in range(share)
    ]
    flip = [(0, 1), (1, 0)]

    def on_device(weights, preact, panel):
        core = lax.axis_index("core")
        first = core == 0
        _, rank, width_in = panel.shape
        width_row = weights.shape[1]
        w1_own, w2_own = weights[0], weights[1]

        partial_out = jnp.einsum("bki,oi->bko", panel, w1_own, preferred_element_type=F32)
        mine = jnp.where(first, partial_out[0], partial_out[1])
        theirs = jnp.where(first, partial_out[1], partial_out[0])
        traded = lax.ppermute(theirs, "core", flip)
        summed_out = mine + traded

        slopes = 1.0 - jnp.tanh(jnp.where(first, preact[0], preact[1])) ** 2
        slope_1 = slopes[0:1]

        cut = width_row // n_x
        y_at, x_at = lax.axis_index("y"), lax.axis_index("x")
        slope_piece = lax.dynamic_slice(slopes[1:2], (0, x_at * cut), (1, cut), allow_negative_indices=False)
        spot = lax.rem(x_at - y_at + n_x, n_x)
        at_turn = lax.broadcasted_iota(jnp.int32, (1, n_x, cut), 1) == spot
        slope_spread = jnp.where(at_turn, slope_piece[:, None], 0.0).reshape(1, width_row)
        slope_rows = jnp.concatenate([*three_parts(slope_spread), jnp.zeros((8 - 3, width_row), BF16)])

        def piece(turn):
            start = lax.rem(y_at + turn, n_x) * cut
            return lax.dynamic_slice(w2_own, (start, 0), (cut, width_in), allow_negative_indices=False)

        kept = jnp.concatenate([piece(core * share + e) for e in range(share)])
        got = lax.ppermute(jnp.concatenate([piece((1 - core) * share + e) for e in range(share)]), "core", flip)
        rows = jnp.concatenate([jnp.where(first, kept, got), jnp.where(first, got, kept)], axis=1)
        rows = [rows[e * cut : (e + 1) * cut] for e in range(share)]
        here = []
        for e in range(share):
            here.append(lax.ppermute(rows[e], ("y", "x", "core"), turns[e]))
        there = [lax.ppermute(block, "core", flip) for block in here]
        blocks = [jnp.where(first, h, t) for h, t in zip(here, there)]
        blocks += [jnp.where(first, t, h) for h, t in zip(here, there)]
        w2 = jnp.concatenate(blocks)
        w1_other = lax.ppermute(w1_own, "core", flip)
        w1, w2 = lax.optimization_barrier((jnp.concatenate([w1_own, w1_other], axis=1), w2))

        image = None
        for iteration in range(ITERS):
            if iteration == 0:
                arrived = to_all(summed_out.astype(BF16), "x", n_x)
                forward = (slope_1 * total(arrived)).astype(BF16)
            else:
                partial_out = dot_t(image, w1).astype(BF16)
                message = jnp.concatenate([partial_out, high_low(dot_t(image, image))], axis=1)
                arrived = to_all(message, "x", n_x)
                forward = normalized_forward(arrived, slope_1, width_row)
            spread = to_all(forward, "z", n_z)
            spread = jnp.moveaxis(spread, 0, 1).reshape(rank, n_z * width_row)
            partial_out = dot_t(spread, w2).astype(BF16)
            if iteration == 0:
                arrived = to_all(jnp.concatenate([partial_out, slope_rows]), "y", n_y)
                slope_2 = total(arrived[:, rank:]).sum(axis=0, keepdims=True)
                arrived = arrived[:, :rank]
            else:
                arrived = to_all(partial_out, "y", n_y)
            forward = (slope_2 * total(arrived)).astype(BF16)
            weighted = (slope_2 * forward.astype(F32)).astype(BF16)
            partial_in = dot_n(weighted, w2).astype(BF16)
            blocks = jnp.moveaxis(partial_in.reshape(rank, n_z, width_row), 1, 0)
            summed = total(exchange(blocks, "z")).astype(BF16)
            cotangent = total(to_all(summed, "x", n_x)).astype(BF16)
            weighted = (slope_1 * cotangent.astype(F32)).astype(BF16)
            partial_in = dot_n(weighted, w1).astype(BF16)
            groups = rank // 8
            cuts = n_y * n_z // groups
            length = 2 * width_in // cuts
            pieces = partial_in.reshape(groups, 8, cuts, length)
            pieces = jnp.moveaxis(pieces, 2, 1).reshape(groups * cuts, 8, length)
            piece = total(exchange(pieces, ("y", "z"))).astype(BF16)
            image = to_all(piece, ("y", "z"), groups * cuts).reshape(groups, cuts, 8, length)
            image = jnp.moveaxis(image, 1, 2).reshape(rank, 2 * width_in)
        there = lax.ppermute(image[:, width_in:], "core", flip)
        arrived = to_all(high_low(dot_t(image, image)), ("x", "core"), 2 * n_x)
        return normalized_panels(core.reshape(1).astype(jnp.int32), arrived, image, there)

    return on_device


def solution(mesh):
    n_x, n_y, n_z = 4, 4, 8
    fine = Mesh(mesh.devices.reshape(n_y, n_z, n_x, 2), ("y", "z", "x", "core"))
    on_device = make(n_x, n_y, n_z)

    return jax.shard_map(
        on_device,
        mesh=fine,
        in_specs=(P(None, ("y", "z"), ("x", "core")), P(None, None, ("y", "z")), P(None, None, ("x", "core"))),
        out_specs=P(None, None, ("x", "core")),
        check_vma=False,
    )
```

```python
import jax
import jax.numpy as jnp
from jax import lax
from jax.experimental import pallas as pl
from jax.experimental.pallas import tpu as pltpu
from jax.sharding import Mesh, PartitionSpec as P


WIDTH = 8192
ITERS = 2
BF16 = jnp.bfloat16
F32 = jnp.float32
WHOLE = pl.BlockSpec(memory_space=pltpu.VMEM)


def on_chip(x):
    return pltpu.with_memory_space_constraint(x, pltpu.VMEM)


def dot_t(a, w):
    return lax.dot_general(a, w, (((1,), (1,)), ((), ())), preferred_element_type=F32)


def dot_n(a, w):
    return lax.dot_general(a, w, (((1,), (0,)), ((), ())), preferred_element_type=F32)


def exchange(tiles, axis):
    return lax.all_to_all(tiles, axis, split_axis=0, concat_axis=0, tiled=True)


def to_all(x, axis, count):
    return exchange(jnp.broadcast_to(x[None], (count, *x.shape)), axis)


def total(tiles):
    return jnp.sum(tiles.astype(F32), axis=0)


def inverse_factors(grams):
    n = grams[0].shape[0]
    count = n // 8
    rows = lax.broadcasted_iota(jnp.int32, (n, n), 0)
    cols = lax.broadcasted_iota(jnp.int32, (n, n), 1)
    eye = (rows == cols).astype(F32)
    row_of = lax.broadcasted_iota(jnp.int32, (8, 2 * n), 0)
    many, across = [], []
    for gram in grams:
        gram = gram * (1.0 / WIDTH)
        diagonal = gram * eye
        down = 1.0 / jnp.sqrt(jnp.sum(diagonal, axis=1, keepdims=True))
        across.append(1.0 / jnp.sqrt(jnp.sum(diagonal, axis=0, keepdims=True)))
        both = jnp.concatenate([eye, gram * down * across[-1]], axis=1)
        many.append([both[8 * i : 8 * i + 8] for i in range(count)])

    def columns_of(blocks, k):
        return [
            {i: jnp.broadcast_to(blocks[i][:, n + 8 * k + t : n + 8 * k + t + 1], (8, 2 * n)) for i in range(k, count)}
            for t in range(8)
        ]

    def step(blocks, columns, scale, k, t):
        live = range(k, count)
        first, second = columns[t], columns[t + 1]
        a, b, d = first[k][t : t + 1], second[k][t : t + 1], second[k][t + 1 : t + 2]
        over_a, over_next = 1.0 / a, a * (1.0 / (a * d - b * b))
        ratio = b * over_a
        second = {i: second[i] - first[i] * ratio for i in live}
        first = dict(first)
        first[k] = jnp.where(row_of > t, first[k], 0.0)
        second[k] = jnp.where(row_of > t + 1, second[k], 0.0)
        for u in range(t + 2, 8):
            entry = columns[u][k][t : t + 1]
            entry_next = (columns[u][k][t + 1 : t + 2] - entry * ratio) * over_next
            entry = entry * over_a
            for i in live:
                columns[u][i] = columns[u][i] - first[i] * entry - second[i] * entry_next
        row = blocks[k][t : t + 1] * over_a
        row_next = (blocks[k][t + 1 : t + 2] - b * row) * over_next
        for i in live:
            blocks[i] = blocks[i] - first[i] * row - second[i] * row_next
        return jnp.where(row_of == t, over_a, jnp.where(row_of == t + 1, over_next, scale))

    done = [[] for _ in many]
    for k in range(count):
        columns = [columns_of(blocks, k) for blocks in many]
        scales = [jnp.zeros((8, 2 * n), F32) for _ in many]
        for t in range(0, 8, 2):
            for g, blocks in enumerate(many):
                scales[g] = step(blocks, columns[g], scales[g], k, t)
        for g, blocks in enumerate(many):
            done[g].append(blocks[k] * jnp.sqrt(scales[g]))
    return [jnp.concatenate(d, axis=0)[:, :n] * s for d, s in zip(done, across)]


def exact_dot(a, b):
    return lax.dot_general(
        a, b, (((1,), (0,)), ((), ())), precision=lax.Precision.HIGHEST, preferred_element_type=F32
    )


def gram_of_parts(parts_ref, start, rank):
    parts = [parts_ref[i, :, start : start + 2 * rank].astype(F32) for i in range(parts_ref.shape[0])]
    summed = parts[0]
    for part in parts[1:]:
        summed = summed + part
    return summed[:, :rank] + summed[:, rank:]


def first_partial(panel, weights):
    inputs, rank, width = panel.shape
    rows = weights.shape[1]

    def kernel(panel_ref, weights_ref, mine_ref, theirs_ref, panel_here, block_here, sems):
        panel_copy = pltpu.make_async_copy(panel_ref, panel_here, sems.at[0])
        block_copy = pltpu.make_async_copy(weights_ref.at[0], block_here, sems.at[1])
        panel_copy.start()
        block_copy.start()
        panel_copy.wait()
        block_copy.wait()
        core = lax.axis_index("core")
        block = block_here[...]
        mine_ref[...] = dot_t(panel_here[pl.ds(core, 1)][0], block)
        theirs_ref[...] = dot_t(panel_here[pl.ds(1 - core, 1)][0], block)

    return pl.pallas_call(
        kernel,
        in_specs=[pl.BlockSpec(memory_space=pltpu.HBM)] * 2,
        out_specs=[WHOLE] * 2,
        out_shape=[pltpu.VMEM((rank, rows), F32)] * 2,
        scratch_shapes=[
            pltpu.VMEM((inputs, rank, width), BF16),
            pltpu.VMEM((rows, width), BF16),
            pltpu.SemaphoreType.DMA((2,)),
        ],
        name="first_partial",
    )(panel, weights)


def normalized_forward(arrived, slope, width):
    count, rank, _ = arrived.shape

    def kernel(arrived_ref, slope_ref, out_ref):
        (inverse,) = inverse_factors([gram_of_parts(arrived_ref, width, rank)])
        summed = arrived_ref[0, :, :width].astype(F32)
        for i in range(1, count):
            summed = summed + arrived_ref[i, :, :width].astype(F32)
        out_ref[...] = (slope_ref[...] * exact_dot(inverse, summed)).astype(BF16)

    return pl.pallas_call(
        kernel,
        in_specs=[WHOLE] * 2,
        out_specs=WHOLE,
        out_shape=pltpu.VMEM((rank, width), BF16),
        name="normalized_forward",
    )(on_chip(arrived), on_chip(slope))


def normalized_panels(core, arrived, image, there):
    rank, width = there.shape

    def kernel(core_ref, arrived_ref, image_ref, there_ref, out_ref):
        here_at = core_ref[0]
        inverses = []
        for b in (here_at, 1 - here_at):
            gram = arrived_ref[pl.ds(b, 1)][0].astype(F32)
            for i in range(2, arrived_ref.shape[0], 2):
                gram = gram + arrived_ref[pl.ds(i + b, 1)][0].astype(F32)
            inverses.append(gram[:, :rank] + gram[:, rank:])
        inverses = inverse_factors(inverses)
        here = exact_dot(inverses[0], image_ref[:, :width].astype(F32))
        out_ref[pl.ds(here_at, 1)] = here[None]
        away = exact_dot(inverses[1], there_ref[...].astype(F32))
        out_ref[pl.ds(1 - here_at, 1)] = away[None]

    return pl.pallas_call(
        kernel,
        in_specs=[pl.BlockSpec(memory_space=pltpu.SMEM)] + [WHOLE] * 3,
        out_specs=WHOLE,
        out_shape=jax.ShapeDtypeStruct((2, rank, width), F32),
        name="normalized_panels",
    )(core, on_chip(arrived), on_chip(image), on_chip(there))


def three_parts(x):
    high = lax.reduce_precision(x, 8, 7)
    middle = lax.reduce_precision(x - high, 8, 7)
    return high.astype(BF16), middle.astype(BF16), (x - high - middle).astype(BF16)


def high_low(gram):
    high = lax.reduce_precision(gram, 8, 7)
    return jnp.concatenate([high.astype(BF16), (gram - high).astype(BF16)], axis=1)


def make(n_x, n_y, n_z):
    share = n_x // 2
    turns = [
        [
            ((i * n_x + j) * 2 + c, (j * n_x + (i + share * c + e) % n_x) * 2 + c)
            for i in range(n_y)
            for j in range(n_x)
            for c in range(2)
        ]
        for e in range(share)
    ]
    flip = [(0, 1), (1, 0)]

    def on_device(weights, preact, panel):
        core = lax.axis_index("core")
        first = core == 0
        _, rank, width_in = panel.shape
        width_row = weights.shape[1]
        w1_own, w2_own = weights[0], weights[1]

        mine, theirs = first_partial(panel, weights)
        traded = lax.ppermute(theirs, "core", flip)
        summed_out = mine + traded

        slopes = 1.0 - jnp.tanh(jnp.where(first, preact[0], preact[1])) ** 2
        slope_1 = slopes[0:1]

        cut = width_row // n_x
        y_at, x_at = lax.axis_index("y"), lax.axis_index("x")
        slope_piece = lax.dynamic_slice(slopes[1:2], (0, x_at * cut), (1, cut), allow_negative_indices=False)
        spot = lax.rem(x_at - y_at + n_x, n_x)
        at_turn = lax.broadcasted_iota(jnp.int32, (1, n_x, cut), 1) == spot
        slope_spread = jnp.where(at_turn, slope_piece[:, None], 0.0).reshape(1, width_row)
        slope_rows = jnp.concatenate([*three_parts(slope_spread), jnp.zeros((8 - 3, width_row), BF16)])

        def piece(turn):
            start = lax.rem(y_at + turn, n_x) * cut
            return lax.dynamic_slice(w2_own, (start, 0), (cut, width_in), allow_negative_indices=False)

        kept = jnp.concatenate([piece(core * share + e) for e in range(share)])
        got = lax.ppermute(jnp.concatenate([piece((1 - core) * share + e) for e in range(share)]), "core", flip)
        rows = jnp.concatenate([jnp.where(first, kept, got), jnp.where(first, got, kept)], axis=1)
        rows = [rows[e * cut : (e + 1) * cut] for e in range(share)]
        here = []
        for e in range(share):
            here.append(lax.ppermute(rows[e], ("y", "x", "core"), turns[e]))
        there = [lax.ppermute(block, "core", flip) for block in here]
        blocks = [jnp.where(first, h, t) for h, t in zip(here, there)]
        blocks += [jnp.where(first, t, h) for h, t in zip(here, there)]
        w2 = jnp.concatenate(blocks)
        w1_other = lax.ppermute(w1_own, "core", flip)
        w1, w2 = lax.optimization_barrier((jnp.concatenate([w1_own, w1_other], axis=1), w2))

        image = None
        for iteration in range(ITERS):
            if iteration == 0:
                arrived = to_all(summed_out.astype(BF16), "x", n_x)
                forward = (slope_1 * total(arrived)).astype(BF16)
            else:
                partial_out = dot_t(image, w1).astype(BF16)
                message = jnp.concatenate([partial_out, high_low(dot_t(image, image))], axis=1)
                arrived = to_all(message, "x", n_x)
                forward = normalized_forward(arrived, slope_1, width_row)
            spread = to_all(forward, "z", n_z)
            spread = jnp.moveaxis(spread, 0, 1).reshape(rank, n_z * width_row)
            partial_out = dot_t(spread, w2).astype(BF16)
            if iteration == 0:
                arrived = to_all(jnp.concatenate([partial_out, slope_rows]), "y", n_y)
                slope_2 = total(arrived[:, rank:]).sum(axis=0, keepdims=True)
                arrived = arrived[:, :rank]
            else:
                arrived = to_all(partial_out, "y", n_y)
            forward = (slope_2 * total(arrived)).astype(BF16)
            weighted = (slope_2 * forward.astype(F32)).astype(BF16)
            partial_in = dot_n(weighted, w2).astype(BF16)
            blocks = jnp.moveaxis(partial_in.reshape(rank, n_z, width_row), 1, 0)
            summed = total(exchange(blocks, "z")).astype(BF16)
            cotangent = total(to_all(summed, "x", n_x)).astype(BF16)
            weighted = (slope_1 * cotangent.astype(F32)).astype(BF16)
            partial_in = dot_n(weighted, w1).astype(BF16)
            groups = rank // 8
            cuts = n_y * n_z // groups
            length = 2 * width_in // cuts
            pieces = partial_in.reshape(groups, 8, cuts, length)
            pieces = jnp.moveaxis(pieces, 2, 1).reshape(groups * cuts, 8, length)
            piece = total(exchange(pieces, ("y", "z"))).astype(BF16)
            image = to_all(piece, ("y", "z"), groups * cuts).reshape(groups, cuts, 8, length)
            image = jnp.moveaxis(image, 1, 2).reshape(rank, 2 * width_in)
        there = lax.ppermute(image[:, width_in:], "core", flip)
        arrived = to_all(high_low(dot_t(image, image)), ("x", "core"), 2 * n_x)
        return normalized_panels(core.reshape(1).astype(jnp.int32), arrived, image, there)

    return on_device


def solution(mesh):
    n_x, n_y, n_z = 4, 4, 8
    fine = Mesh(mesh.devices.reshape(n_y, n_z, n_x, 2), ("y", "z", "x", "core"))
    on_device = make(n_x, n_y, n_z)

    return jax.shard_map(
        on_device,
        mesh=fine,
        in_specs=(P(None, ("y", "z"), ("x", "core")), P(None, None, ("y", "z")), P(None, None, ("x", "core"))),
        out_specs=P(None, None, ("x", "core")),
        check_vma=False,
    )
```

```python
import jax
import jax.numpy as jnp
from jax import lax
from jax.experimental import pallas as pl
from jax.experimental.pallas import tpu as pltpu
from jax.sharding import Mesh, PartitionSpec as P


WIDTH = 8192
ITERS = 2
BF16 = jnp.bfloat16
F32 = jnp.float32
WHOLE = pl.BlockSpec(memory_space=pltpu.VMEM)


def on_chip(x):
    return pltpu.with_memory_space_constraint(x, pltpu.VMEM)


def dot_t(a, w):
    return lax.dot_general(a, w, (((1,), (1,)), ((), ())), preferred_element_type=F32)


def dot_n(a, w):
    return lax.dot_general(a, w, (((1,), (0,)), ((), ())), preferred_element_type=F32)


def exchange(tiles, axis):
    return lax.all_to_all(tiles, axis, split_axis=0, concat_axis=0, tiled=True)


def to_all(x, axis, count):
    return exchange(jnp.broadcast_to(x[None], (count, *x.shape)), axis)


def total(tiles):
    return jnp.sum(tiles.astype(F32), axis=0)


def inverse_factors(grams):
    n = grams[0].shape[0]
    count = n // 8
    rows = lax.broadcasted_iota(jnp.int32, (n, n), 0)
    cols = lax.broadcasted_iota(jnp.int32, (n, n), 1)
    eye = (rows == cols).astype(F32)
    row_of = lax.broadcasted_iota(jnp.int32, (8, 2 * n), 0)
    many, across = [], []
    for gram in grams:
        gram = gram * (1.0 / WIDTH)
        diagonal = gram * eye
        down = 1.0 / jnp.sqrt(jnp.sum(diagonal, axis=1, keepdims=True))
        across.append(1.0 / jnp.sqrt(jnp.sum(diagonal, axis=0, keepdims=True)))
        both = jnp.concatenate([eye, gram * down * across[-1]], axis=1)
        many.append([both[8 * i : 8 * i + 8] for i in range(count)])

    def columns_of(blocks, k):
        return [
            {i: jnp.broadcast_to(blocks[i][:, n + 8 * k + t : n + 8 * k + t + 1], (8, 2 * n)) for i in range(k, count)}
            for t in range(8)
        ]

    def step(blocks, columns, scale, k, t):
        live = range(k, count)
        first, second = columns[t], columns[t + 1]
        a, b, d = first[k][t : t + 1], second[k][t : t + 1], second[k][t + 1 : t + 2]
        over_a, over_next = 1.0 / a, a * (1.0 / (a * d - b * b))
        ratio = b * over_a
        second = {i: second[i] - first[i] * ratio for i in live}
        first = dict(first)
        first[k] = jnp.where(row_of > t, first[k], 0.0)
        second[k] = jnp.where(row_of > t + 1, second[k], 0.0)
        for u in range(t + 2, 8):
            entry = columns[u][k][t : t + 1]
            entry_next = (columns[u][k][t + 1 : t + 2] - entry * ratio) * over_next
            entry = entry * over_a
            for i in live:
                columns[u][i] = columns[u][i] - first[i] * entry - second[i] * entry_next
        row = blocks[k][t : t + 1] * over_a
        row_next = (blocks[k][t + 1 : t + 2] - b * row) * over_next
        for i in live:
            blocks[i] = blocks[i] - first[i] * row - second[i] * row_next
        return jnp.where(row_of == t, over_a, jnp.where(row_of == t + 1, over_next, scale))

    done = [[] for _ in many]
    for k in range(count):
        columns = [columns_of(blocks, k) for blocks in many]
        scales = [jnp.zeros((8, 2 * n), F32) for _ in many]
        for t in range(0, 8, 2):
            for g, blocks in enumerate(many):
                scales[g] = step(blocks, columns[g], scales[g], k, t)
        for g, blocks in enumerate(many):
            done[g].append(blocks[k] * jnp.sqrt(scales[g]))
    return [jnp.concatenate(d, axis=0)[:, :n] * s for d, s in zip(done, across)]


def exact_dot(a, b):
    return lax.dot_general(
        a, b, (((1,), (0,)), ((), ())), precision=lax.Precision.HIGHEST, preferred_element_type=F32
    )


def gram_of_parts(parts_ref, start, rank):
    parts = [parts_ref[i, :, start : start + 2 * rank].astype(F32) for i in range(parts_ref.shape[0])]
    summed = parts[0]
    for part in parts[1:]:
        summed = summed + part
    return summed[:, :rank] + summed[:, rank:]


def first_partial(panel, weights):
    inputs, rank, width = panel.shape
    rows = weights.shape[1]

    def kernel(panel_ref, weights_ref, mine_ref, theirs_ref, panel_here, block_here, sems):
        panel_copy = pltpu.make_async_copy(panel_ref, panel_here, sems.at[0])
        block_copy = pltpu.make_async_copy(weights_ref.at[0], block_here, sems.at[1])
        panel_copy.start()
        block_copy.start()
        panel_copy.wait()
        block_copy.wait()
        core = lax.axis_index("core")
        block = block_here[...]
        mine_ref[...] = dot_t(panel_here[pl.ds(core, 1)][0], block)
        theirs_ref[...] = dot_t(panel_here[pl.ds(1 - core, 1)][0], block)

    return pl.pallas_call(
        kernel,
        in_specs=[pl.BlockSpec(memory_space=pltpu.HBM)] * 2,
        out_specs=[WHOLE] * 2,
        out_shape=[pltpu.VMEM((rank, rows), F32)] * 2,
        scratch_shapes=[
            pltpu.VMEM((inputs, rank, width), BF16),
            pltpu.VMEM((rows, width), BF16),
            pltpu.SemaphoreType.DMA((2,)),
        ],
        name="first_partial",
    )(panel, weights)


def normalized_forward(arrived, slope, width):
    count, rank, _ = arrived.shape

    def kernel(arrived_ref, slope_ref, out_ref):
        (inverse,) = inverse_factors([gram_of_parts(arrived_ref, width, rank)])
        summed = arrived_ref[0, :, :width].astype(F32)
        for i in range(1, count):
            summed = summed + arrived_ref[i, :, :width].astype(F32)
        out_ref[...] = (slope_ref[...] * exact_dot(inverse, summed)).astype(BF16)

    return pl.pallas_call(
        kernel,
        in_specs=[WHOLE] * 2,
        out_specs=WHOLE,
        out_shape=pltpu.VMEM((rank, width), BF16),
        name="normalized_forward",
    )(on_chip(arrived), on_chip(slope))


def normalized_panels(arrived, image, there):
    rank, width = there.shape

    def times(inverse, panel):
        high = inverse.astype(BF16)
        rest = inverse - high.astype(F32)
        middle = rest.astype(BF16)
        low = (rest - middle.astype(F32)).astype(BF16)
        products = dot_n(jnp.concatenate([high, middle, low]), panel)
        return products[:rank] + (products[rank : 2 * rank] + products[2 * rank :])

    def kernel(arrived_ref, image_ref, there_ref, out_ref, result, sems):
        here_at = lax.axis_index("core")
        inverses = []
        for b in (here_at, 1 - here_at):
            gram = arrived_ref[pl.ds(b, 1)][0].astype(F32)
            for i in range(2, arrived_ref.shape[0], 2):
                gram = gram + arrived_ref[pl.ds(i + b, 1)][0].astype(F32)
            inverses.append(gram[:, :rank] + gram[:, rank:])
        inverses = inverse_factors(inverses)
        result[0] = times(inverses[0], image_ref[:, :width])
        first = pltpu.make_async_copy(result.at[0], out_ref.at[here_at], sems.at[0])
        first.start()
        result[1] = times(inverses[1], there_ref[...])
        second = pltpu.make_async_copy(result.at[1], out_ref.at[1 - here_at], sems.at[1])
        second.start()
        first.wait()
        second.wait()

    return pl.pallas_call(
        kernel,
        in_specs=[WHOLE] * 3,
        out_specs=pl.BlockSpec(memory_space=pltpu.HBM),
        out_shape=jax.ShapeDtypeStruct((2, rank, width), F32),
        scratch_shapes=[pltpu.VMEM((2, rank, width), F32), pltpu.SemaphoreType.DMA((2,))],
        name="normalized_panels",
    )(on_chip(arrived), on_chip(image), on_chip(there))


def three_parts(x):
    high = lax.reduce_precision(x, 8, 7)
    middle = lax.reduce_precision(x - high, 8, 7)
    return high.astype(BF16), middle.astype(BF16), (x - high - middle).astype(BF16)


def high_low(gram):
    high = lax.reduce_precision(gram, 8, 7)
    return jnp.concatenate([high.astype(BF16), (gram - high).astype(BF16)], axis=1)


def make(n_x, n_y, n_z):
    share = n_x // 2
    turns = [
        [
            ((i * n_x + j) * 2 + c, (j * n_x + (i + share * c + e) % n_x) * 2 + c)
            for i in range(n_y)
            for j in range(n_x)
            for c in range(2)
        ]
        for e in range(share)
    ]
    flip = [(0, 1), (1, 0)]
    near, far = [(i, i ^ 1) for i in range(n_x)], [(i, n_x - 1 - i) for i in range(n_x)]

    def on_device(weights, preact, panel):
        core = lax.axis_index("core")
        first = core == 0
        _, rank, width_in = panel.shape
        width_row = weights.shape[1]
        w1_own, w2_own = weights[0], weights[1]

        mine, theirs = first_partial(panel, weights)
        traded = lax.ppermute(theirs, "core", flip)
        summed_out = mine + traded

        slopes = 1.0 - jnp.tanh(jnp.where(first, preact[0], preact[1])) ** 2
        slope_1 = slopes[0:1]

        cut = width_row // n_x
        y_at, x_at = lax.axis_index("y"), lax.axis_index("x")
        slope_piece = lax.dynamic_slice(slopes[1:2], (0, x_at * cut), (1, cut), allow_negative_indices=False)
        spot = lax.rem(x_at - y_at + n_x, n_x)
        at_turn = lax.broadcasted_iota(jnp.int32, (1, n_x, cut), 1) == spot
        slope_spread = jnp.where(at_turn, slope_piece[:, None], 0.0).reshape(1, width_row)
        slope_rows = jnp.concatenate([*three_parts(slope_spread), jnp.zeros((8 - 3, width_row), BF16)])

        def piece(turn):
            start = lax.rem(y_at + turn, n_x) * cut
            return lax.dynamic_slice(w2_own, (start, 0), (cut, width_in), allow_negative_indices=False)

        kept = jnp.concatenate([piece(core * share + e) for e in range(share)])
        got = lax.ppermute(jnp.concatenate([piece((1 - core) * share + e) for e in range(share)]), "core", flip)
        rows = jnp.concatenate([jnp.where(first, kept, got), jnp.where(first, got, kept)], axis=1)
        rows = [rows[e * cut : (e + 1) * cut] for e in range(share)]
        here = []
        for e in range(share):
            here.append(lax.ppermute(rows[e], ("y", "x", "core"), turns[e]))
        there = [lax.ppermute(block, "core", flip) for block in here]
        blocks = [jnp.where(first, h, t) for h, t in zip(here, there)]
        blocks += [jnp.where(first, t, h) for h, t in zip(here, there)]
        w2 = jnp.concatenate(blocks)
        w1_other = lax.ppermute(w1_own, "core", flip)
        w1, w2 = lax.optimization_barrier((jnp.concatenate([w1_own, w1_other], axis=1), w2))

        image = None
        for iteration in range(ITERS):
            if iteration == 0:
                arrived = to_all(summed_out.astype(BF16), "x", n_x)
                forward = (slope_1 * total(arrived)).astype(BF16)
            else:
                partial_out = dot_t(image, w1).astype(BF16)
                message = jnp.concatenate([partial_out, high_low(dot_t(image, image))], axis=1)
                arrived = to_all(message, "x", n_x)
                forward = normalized_forward(arrived, slope_1, width_row)
            spread = to_all(forward, "z", n_z)
            spread = jnp.moveaxis(spread, 0, 1).reshape(rank, n_z * width_row)
            partial_out = dot_t(spread, w2).astype(BF16)
            if iteration == 0:
                arrived = to_all(jnp.concatenate([partial_out, slope_rows]), "y", n_y)
                slope_2 = total(arrived[:, rank:]).sum(axis=0, keepdims=True)
                arrived = arrived[:, :rank]
            else:
                arrived = to_all(partial_out, "y", n_y)
            forward = (slope_2 * total(arrived)).astype(BF16)
            weighted = (slope_2 * forward.astype(F32)).astype(BF16)
            partial_in = dot_n(weighted, w2).astype(BF16)
            blocks = jnp.moveaxis(partial_in.reshape(rank, n_z, width_row), 1, 0)
            summed = total(exchange(blocks, "z")).astype(BF16)
            for step in (near, far):
                there = lax.ppermute(summed, "x", step)
                summed = (summed.astype(F32) + there.astype(F32)).astype(BF16)
            cotangent = summed
            weighted = (slope_1 * cotangent.astype(F32)).astype(BF16)
            partial_in = dot_n(weighted, w1).astype(BF16)
            groups = rank // 8
            cuts = n_y * n_z // groups
            length = 2 * width_in // cuts
            pieces = partial_in.reshape(groups, 8, cuts, length)
            pieces = jnp.moveaxis(pieces, 2, 1).reshape(groups * cuts, 8, length)
            piece = total(exchange(pieces, ("y", "z"))).astype(BF16)
            image = to_all(piece, ("y", "z"), groups * cuts).reshape(groups, cuts, 8, length)
            image = jnp.moveaxis(image, 1, 2).reshape(rank, 2 * width_in)
        there = lax.ppermute(image[:, width_in:], "core", flip)
        arrived = to_all(high_low(dot_t(image, image)), ("x", "core"), 2 * n_x)
        return normalized_panels(arrived, image, there)

    return on_device


def solution(mesh):
    n_x, n_y, n_z = 4, 4, 8
    fine = Mesh(mesh.devices.reshape(n_y, n_z, n_x, 2), ("y", "z", "x", "core"))
    on_device = make(n_x, n_y, n_z)

    return jax.shard_map(
        on_device,
        mesh=fine,
        in_specs=(P(None, ("y", "z"), ("x", "core")), P(None, None, ("y", "z")), P(None, None, ("x", "core"))),
        out_specs=P(None, None, ("x", "core")),
        check_vma=False,
    )
```

```python
import jax
import jax.numpy as jnp
from jax import lax
from jax.experimental import pallas as pl
from jax.experimental.pallas import tpu as pltpu
from jax.sharding import Mesh, PartitionSpec as P


WIDTH = 8192
ITERS = 2
BF16 = jnp.bfloat16
F32 = jnp.float32
WHOLE = pl.BlockSpec(memory_space=pltpu.VMEM)


def on_chip(x):
    return pltpu.with_memory_space_constraint(x, pltpu.VMEM)


def dot_t(a, w):
    return lax.dot_general(a, w, (((1,), (1,)), ((), ())), preferred_element_type=F32)


def dot_n(a, w):
    return lax.dot_general(a, w, (((1,), (0,)), ((), ())), preferred_element_type=F32)


def exchange(tiles, axis):
    return lax.all_to_all(tiles, axis, split_axis=0, concat_axis=0, tiled=True)


def to_all(x, axis, count):
    return exchange(jnp.broadcast_to(x[None], (count, *x.shape)), axis)


def total(tiles):
    return jnp.sum(tiles.astype(F32), axis=0)


def inverse_factors(grams):
    n = grams[0].shape[0]
    count = n // 8
    rows = lax.broadcasted_iota(jnp.int32, (n, n), 0)
    cols = lax.broadcasted_iota(jnp.int32, (n, n), 1)
    eye = (rows == cols).astype(F32)
    row_of = lax.broadcasted_iota(jnp.int32, (8, 2 * n), 0)
    many, across = [], []
    for gram in grams:
        gram = gram * (1.0 / WIDTH)
        diagonal = gram * eye
        down = 1.0 / jnp.sqrt(jnp.sum(diagonal, axis=1, keepdims=True))
        across.append(1.0 / jnp.sqrt(jnp.sum(diagonal, axis=0, keepdims=True)))
        both = jnp.concatenate([eye, gram * down * across[-1]], axis=1)
        many.append([both[8 * i : 8 * i + 8] for i in range(count)])

    def columns_of(blocks, k):
        return [
            {i: jnp.broadcast_to(blocks[i][:, n + 8 * k + t : n + 8 * k + t + 1], (8, 2 * n)) for i in range(k, count)}
            for t in range(8)
        ]

    def step(blocks, columns, scale, k, t):
        live = range(k, count)
        first, second = columns[t], columns[t + 1]
        a, b, d = first[k][t : t + 1], second[k][t : t + 1], second[k][t + 1 : t + 2]
        over_a, over_next = 1.0 / a, a * (1.0 / (a * d - b * b))
        ratio = b * over_a
        second = {i: second[i] - first[i] * ratio for i in live}
        first = dict(first)
        first[k] = jnp.where(row_of > t, first[k], 0.0)
        second[k] = jnp.where(row_of > t + 1, second[k], 0.0)
        for u in range(t + 2, 8):
            entry = columns[u][k][t : t + 1]
            entry_next = (columns[u][k][t + 1 : t + 2] - entry * ratio) * over_next
            entry = entry * over_a
            for i in live:
                columns[u][i] = columns[u][i] - first[i] * entry - second[i] * entry_next
        row = blocks[k][t : t + 1] * over_a
        row_next = (blocks[k][t + 1 : t + 2] - b * row) * over_next
        for i in live:
            blocks[i] = blocks[i] - first[i] * row - second[i] * row_next
        return jnp.where(row_of == t, over_a, jnp.where(row_of == t + 1, over_next, scale))

    done = [[] for _ in many]
    for k in range(count):
        columns = [columns_of(blocks, k) for blocks in many]
        scales = [jnp.zeros((8, 2 * n), F32) for _ in many]
        for t in range(0, 8, 2):
            for g, blocks in enumerate(many):
                scales[g] = step(blocks, columns[g], scales[g], k, t)
        for g, blocks in enumerate(many):
            done[g].append(blocks[k] * jnp.sqrt(scales[g]))
    return [jnp.concatenate(d, axis=0)[:, :n] * s for d, s in zip(done, across)]


def exact_dot(a, b):
    return lax.dot_general(
        a, b, (((1,), (0,)), ((), ())), precision=lax.Precision.HIGHEST, preferred_element_type=F32
    )


def gram_of_parts(parts_ref, start, rank):
    parts = [parts_ref[i, :rank, start : start + 2 * rank].astype(F32) for i in range(parts_ref.shape[0])]
    summed = parts[0]
    for part in parts[1:]:
        summed = summed + part
    return summed[:, :rank] + summed[:, rank:]


def first_partial(panel, weights):
    inputs, rank, width = panel.shape
    rows = weights.shape[1]

    def kernel(panel_ref, weights_ref, mine_ref, theirs_ref, panel_here, block_here, sems):
        panel_copy = pltpu.make_async_copy(panel_ref, panel_here, sems.at[0])
        block_copy = pltpu.make_async_copy(weights_ref.at[0], block_here, sems.at[1])
        panel_copy.start()
        block_copy.start()
        panel_copy.wait()
        block_copy.wait()
        core = lax.axis_index("core")
        block = block_here[...]
        mine_ref[...] = dot_t(panel_here[pl.ds(core, 1)][0], block)
        theirs_ref[...] = dot_t(panel_here[pl.ds(1 - core, 1)][0], block)

    return pl.pallas_call(
        kernel,
        in_specs=[pl.BlockSpec(memory_space=pltpu.HBM)] * 2,
        out_specs=[WHOLE] * 2,
        out_shape=[pltpu.VMEM((rank, rows), F32)] * 2,
        scratch_shapes=[
            pltpu.VMEM((inputs, rank, width), BF16),
            pltpu.VMEM((rows, width), BF16),
            pltpu.SemaphoreType.DMA((2,)),
        ],
        name="first_partial",
    )(panel, weights)


def normalized_forward(arrived, slope, width):
    count, rank = arrived.shape[0], arrived.shape[1] - 8

    def kernel(arrived_ref, slope_ref, out_ref):
        (inverse,) = inverse_factors([gram_of_parts(arrived_ref, width, rank)])
        summed = arrived_ref[0, :rank, :width].astype(F32)
        for i in range(1, count):
            summed = summed + arrived_ref[i, :rank, :width].astype(F32)
        out_ref[...] = (slope_ref[...] * exact_dot(inverse, summed)).astype(BF16)

    return pl.pallas_call(
        kernel,
        in_specs=[WHOLE] * 2,
        out_specs=WHOLE,
        out_shape=pltpu.VMEM((rank, width), BF16),
        name="normalized_forward",
    )(on_chip(arrived), on_chip(slope))


def normalized_panels(arrived, image, there):
    rank, width = there.shape

    def times(inverse, panel):
        high = inverse.astype(BF16)
        rest = inverse - high.astype(F32)
        middle = rest.astype(BF16)
        low = (rest - middle.astype(F32)).astype(BF16)
        products = dot_n(jnp.concatenate([high, middle, low]), panel)
        return products[:rank] + (products[rank : 2 * rank] + products[2 * rank :])

    def kernel(arrived_ref, image_ref, there_ref, out_ref, result, sems):
        here_at = lax.axis_index("core")
        inverses = []
        for b in (here_at, 1 - here_at):
            gram = arrived_ref[pl.ds(b, 1)][0].astype(F32)
            for i in range(2, arrived_ref.shape[0], 2):
                gram = gram + arrived_ref[pl.ds(i + b, 1)][0].astype(F32)
            inverses.append(gram[:, :rank] + gram[:, rank:])
        inverses = inverse_factors(inverses)
        result[0] = times(inverses[0], image_ref[:, :width])
        first = pltpu.make_async_copy(result.at[0], out_ref.at[here_at], sems.at[0])
        first.start()
        result[1] = times(inverses[1], there_ref[...])
        second = pltpu.make_async_copy(result.at[1], out_ref.at[1 - here_at], sems.at[1])
        second.start()
        first.wait()
        second.wait()

    return pl.pallas_call(
        kernel,
        in_specs=[WHOLE] * 3,
        out_specs=pl.BlockSpec(memory_space=pltpu.HBM),
        out_shape=jax.ShapeDtypeStruct((2, rank, width), F32),
        scratch_shapes=[pltpu.VMEM((2, rank, width), F32), pltpu.SemaphoreType.DMA((2,))],
        name="normalized_panels",
    )(on_chip(arrived), on_chip(image), on_chip(there))


def three_parts(x):
    high = lax.reduce_precision(x, 8, 7)
    middle = lax.reduce_precision(x - high, 8, 7)
    return high.astype(BF16), middle.astype(BF16), (x - high - middle).astype(BF16)


def high_low(gram):
    high = lax.reduce_precision(gram, 8, 7)
    return jnp.concatenate([high.astype(BF16), (gram - high).astype(BF16)], axis=1)


def make(n_x, n_y, n_z):
    share = n_x // 2
    turns = [
        [
            ((i * n_x + j) * 2 + c, (j * n_x + (i + share * c + e) % n_x) * 2 + c)
            for i in range(n_y)
            for j in range(n_x)
            for c in range(2)
        ]
        for e in range(share)
    ]
    flip = [(0, 1), (1, 0)]

    def on_device(weights, preact, panel):
        core = lax.axis_index("core")
        first = core == 0
        _, rank, width_in = panel.shape
        width_row = weights.shape[1]
        w1_own, w2_own = weights[0], weights[1]

        mine, theirs = first_partial(panel, weights)
        traded = lax.ppermute(theirs, "core", flip)
        summed_out = mine + traded

        slopes = 1.0 - jnp.tanh(jnp.where(first, preact[0], preact[1])) ** 2
        slope_1 = slopes[0:1]

        cut = width_row // n_x
        y_at, x_at = lax.axis_index("y"), lax.axis_index("x")
        slope_piece = lax.dynamic_slice(slopes[1:2], (0, x_at * cut), (1, cut), allow_negative_indices=False)
        spot = lax.rem(x_at - y_at + n_x, n_x)
        at_turn = lax.broadcasted_iota(jnp.int32, (1, n_x, cut), 1) == spot
        slope_spread = jnp.where(at_turn, slope_piece[:, None], 0.0).reshape(1, width_row)
        slope_rows = jnp.concatenate([*three_parts(slope_spread), jnp.zeros((8 - 3, width_row), BF16)])

        def piece(turn):
            start = lax.rem(y_at + turn, n_x) * cut
            return lax.dynamic_slice(w2_own, (start, 0), (cut, width_in), allow_negative_indices=False)

        kept = jnp.concatenate([piece(core * share + e) for e in range(share)])
        got = lax.ppermute(jnp.concatenate([piece((1 - core) * share + e) for e in range(share)]), "core", flip)
        rows = jnp.concatenate([jnp.where(first, kept, got), jnp.where(first, got, kept)], axis=1)
        rows = [rows[e * cut : (e + 1) * cut] for e in range(share)]
        here = []
        for e in range(share):
            here.append(lax.ppermute(rows[e], ("y", "x", "core"), turns[e]))
        there = [lax.ppermute(block, "core", flip) for block in here]
        blocks = [jnp.where(first, h, t) for h, t in zip(here, there)]
        blocks += [jnp.where(first, t, h) for h, t in zip(here, there)]
        w2 = jnp.concatenate(blocks)
        w1_other = lax.ppermute(w1_own, "core", flip)
        w1, w2 = lax.optimization_barrier((jnp.concatenate([w1_own, w1_other], axis=1), w2))

        image = None
        for iteration in range(ITERS):
            if iteration == 0:
                arrived = to_all(summed_out.astype(BF16), "x", n_x)
                forward = (slope_1 * total(arrived)).astype(BF16)
            else:
                paced = lax.ppermute(image[:8, : width_row + 2 * rank], "core", flip)
                partial_out = dot_t(image, w1).astype(BF16)
                message = jnp.concatenate([partial_out, high_low(dot_t(image, image))], axis=1)
                message = jnp.concatenate([message, paced])
                arrived = to_all(message, "x", n_x)
                forward = normalized_forward(arrived, slope_1, width_row)
            spread = to_all(forward, "z", n_z)
            spread = jnp.moveaxis(spread, 0, 1).reshape(rank, n_z * width_row)
            partial_out = dot_t(spread, w2).astype(BF16)
            if iteration == 0:
                arrived = to_all(jnp.concatenate([partial_out, slope_rows]), "y", n_y)
                slope_2 = total(arrived[:, rank:]).sum(axis=0, keepdims=True)
                arrived = arrived[:, :rank]
            else:
                arrived = to_all(partial_out, "y", n_y)
            forward = (slope_2 * total(arrived)).astype(BF16)
            weighted = (slope_2 * forward.astype(F32)).astype(BF16)
            partial_in = dot_n(weighted, w2).astype(BF16)
            blocks = jnp.moveaxis(partial_in.reshape(rank, n_z, width_row), 1, 0)
            summed = total(exchange(blocks, "z")).astype(BF16)
            cotangent = total(to_all(summed, "x", n_x)).astype(BF16)
            weighted = (slope_1 * cotangent.astype(F32)).astype(BF16)
            partial_in = dot_n(weighted, w1).astype(BF16)
            groups = rank // 8
            cuts = n_y * n_z // groups
            length = 2 * width_in // cuts
            pieces = partial_in.reshape(groups, 8, cuts, length)
            pieces = jnp.moveaxis(pieces, 2, 1).reshape(groups * cuts, 8, length)
            piece = total(exchange(pieces, ("y", "z"))).astype(BF16)
            image = to_all(piece, ("y", "z"), groups * cuts).reshape(groups, cuts, 8, length)
            image = jnp.moveaxis(image, 1, 2).reshape(rank, 2 * width_in)
        there = lax.ppermute(image[:, width_in:], "core", flip)
        arrived = to_all(high_low(dot_t(image, image)), ("x", "core"), 2 * n_x)
        return normalized_panels(arrived, image, there)

    return on_device


def solution(mesh):
    n_x, n_y, n_z = 4, 4, 8
    fine = Mesh(mesh.devices.reshape(n_y, n_z, n_x, 2), ("y", "z", "x", "core"))
    on_device = make(n_x, n_y, n_z)

    return jax.shard_map(
        on_device,
        mesh=fine,
        in_specs=(P(None, ("y", "z"), ("x", "core")), P(None, None, ("y", "z")), P(None, None, ("x", "core"))),
        out_specs=P(None, None, ("x", "core")),
        check_vma=False,
    )
```

```python
import jax
import jax.numpy as jnp
from jax import lax
from jax.experimental import pallas as pl
from jax.experimental.pallas import tpu as pltpu
from jax.sharding import Mesh, PartitionSpec as P


WIDTH = 8192
ITERS = 2
BF16 = jnp.bfloat16
F32 = jnp.float32
WHOLE = pl.BlockSpec(memory_space=pltpu.VMEM)


def on_chip(x):
    return pltpu.with_memory_space_constraint(x, pltpu.VMEM)


def dot_t(a, w):
    return lax.dot_general(a, w, (((1,), (1,)), ((), ())), preferred_element_type=F32)


def dot_n(a, w):
    return lax.dot_general(a, w, (((1,), (0,)), ((), ())), preferred_element_type=F32)


def exchange(tiles, axis):
    return lax.all_to_all(tiles, axis, split_axis=0, concat_axis=0, tiled=True)


def to_all(x, axis, count):
    return exchange(jnp.broadcast_to(x[None], (count, *x.shape)), axis)


def total(tiles):
    return jnp.sum(tiles.astype(F32), axis=0)


def inverse_factors(grams):
    n = grams[0].shape[0]
    count = n // 8
    rows = lax.broadcasted_iota(jnp.int32, (n, n), 0)
    cols = lax.broadcasted_iota(jnp.int32, (n, n), 1)
    eye = (rows == cols).astype(F32)
    row_of = lax.broadcasted_iota(jnp.int32, (8, 2 * n), 0)
    many, across = [], []
    for gram in grams:
        gram = gram * (1.0 / WIDTH)
        diagonal = gram * eye
        down = 1.0 / jnp.sqrt(jnp.sum(diagonal, axis=1, keepdims=True))
        across.append(1.0 / jnp.sqrt(jnp.sum(diagonal, axis=0, keepdims=True)))
        both = jnp.concatenate([eye, gram * down * across[-1]], axis=1)
        many.append([both[8 * i : 8 * i + 8] for i in range(count)])

    def columns_of(blocks, k):
        return [
            {i: jnp.broadcast_to(blocks[i][:, n + 8 * k + t : n + 8 * k + t + 1], (8, 2 * n)) for i in range(k, count)}
            for t in range(8)
        ]

    def step(blocks, columns, scale, k, t):
        live = range(k, count)
        first, second = columns[t], columns[t + 1]
        a, b, d = first[k][t : t + 1], second[k][t : t + 1], second[k][t + 1 : t + 2]
        over_a, over_next = 1.0 / a, a * (1.0 / (a * d - b * b))
        ratio = b * over_a
        second = {i: second[i] - first[i] * ratio for i in live}
        first = dict(first)
        first[k] = jnp.where(row_of > t, first[k], 0.0)
        second[k] = jnp.where(row_of > t + 1, second[k], 0.0)
        for u in range(t + 2, 8):
            entry = columns[u][k][t : t + 1]
            entry_next = (columns[u][k][t + 1 : t + 2] - entry * ratio) * over_next
            entry = entry * over_a
            for i in live:
                columns[u][i] = columns[u][i] - first[i] * entry - second[i] * entry_next
        row = blocks[k][t : t + 1] * over_a
        row_next = (blocks[k][t + 1 : t + 2] - b * row) * over_next
        for i in live:
            blocks[i] = blocks[i] - first[i] * row - second[i] * row_next
        return jnp.where(row_of == t, over_a, jnp.where(row_of == t + 1, over_next, scale))

    done = [[] for _ in many]
    for k in range(count):
        columns = [columns_of(blocks, k) for blocks in many]
        scales = [jnp.zeros((8, 2 * n), F32) for _ in many]
        for t in range(0, 8, 2):
            for g, blocks in enumerate(many):
                scales[g] = step(blocks, columns[g], scales[g], k, t)
        for g, blocks in enumerate(many):
            done[g].append(blocks[k] * jnp.sqrt(scales[g]))
    return [jnp.concatenate(d, axis=0)[:, :n] * s for d, s in zip(done, across)]


def exact_dot(a, b):
    return lax.dot_general(
        a, b, (((1,), (0,)), ((), ())), precision=lax.Precision.HIGHEST, preferred_element_type=F32
    )


def gram_of_parts(parts_ref, start, rank):
    parts = [parts_ref[i, :, start : start + 2 * rank].astype(F32) for i in range(parts_ref.shape[0])]
    summed = parts[0]
    for part in parts[1:]:
        summed = summed + part
    return summed[:, :rank] + summed[:, rank:]


def first_partial(panel, weights):
    inputs, rank, width = panel.shape
    rows = weights.shape[1]

    def kernel(panel_ref, weights_ref, mine_ref, theirs_ref, panel_here, block_here, sems):
        panel_copy = pltpu.make_async_copy(panel_ref, panel_here, sems.at[0])
        block_copy = pltpu.make_async_copy(weights_ref.at[0], block_here, sems.at[1])
        panel_copy.start()
        block_copy.start()
        panel_copy.wait()
        block_copy.wait()
        core = lax.axis_index("core")
        block = block_here[...]
        mine_ref[...] = dot_t(panel_here[pl.ds(core, 1)][0], block)
        theirs_ref[...] = dot_t(panel_here[pl.ds(1 - core, 1)][0], block)

    return pl.pallas_call(
        kernel,
        in_specs=[pl.BlockSpec(memory_space=pltpu.HBM)] * 2,
        out_specs=[WHOLE] * 2,
        out_shape=[pltpu.VMEM((rank, rows), F32)] * 2,
        scratch_shapes=[
            pltpu.VMEM((inputs, rank, width), BF16),
            pltpu.VMEM((rows, width), BF16),
            pltpu.SemaphoreType.DMA((2,)),
        ],
        name="first_partial",
    )(panel, weights)


def normalized_forward(arrived, slope, width):
    count, rank, _ = arrived.shape

    def kernel(arrived_ref, slope_ref, out_ref):
        (inverse,) = inverse_factors([gram_of_parts(arrived_ref, width, rank)])
        summed = arrived_ref[0, :, :width].astype(F32)
        for i in range(1, count):
            summed = summed + arrived_ref[i, :, :width].astype(F32)
        out_ref[...] = (slope_ref[...] * exact_dot(inverse, summed)).astype(BF16)

    return pl.pallas_call(
        kernel,
        in_specs=[WHOLE] * 2,
        out_specs=WHOLE,
        out_shape=pltpu.VMEM((rank, width), BF16),
        name="normalized_forward",
    )(on_chip(arrived), on_chip(slope))


def normalized_panels(arrived, image, there):
    rank, width = there.shape

    def times(inverse, panel):
        high = inverse.astype(BF16)
        rest = inverse - high.astype(F32)
        middle = rest.astype(BF16)
        low = (rest - middle.astype(F32)).astype(BF16)
        products = dot_n(jnp.concatenate([high, middle, low]), panel)
        return products[:rank] + (products[rank : 2 * rank] + products[2 * rank :])

    def kernel(arrived_ref, image_ref, there_ref, out_ref, result, sems):
        here_at = lax.axis_index("core")
        inverses = []
        for b in (here_at, 1 - here_at):
            gram = arrived_ref[pl.ds(b, 1)][0].astype(F32)
            for i in range(2, arrived_ref.shape[0], 2):
                gram = gram + arrived_ref[pl.ds(i + b, 1)][0].astype(F32)
            inverses.append(gram[:, :rank] + gram[:, rank:])
        inverses = inverse_factors(inverses)
        result[0] = times(inverses[0], image_ref[:, :width])
        first = pltpu.make_async_copy(result.at[0], out_ref.at[here_at], sems.at[0])
        first.start()
        result[1] = times(inverses[1], there_ref[...])
        second = pltpu.make_async_copy(result.at[1], out_ref.at[1 - here_at], sems.at[1])
        second.start()
        first.wait()
        second.wait()

    return pl.pallas_call(
        kernel,
        in_specs=[WHOLE] * 3,
        out_specs=pl.BlockSpec(memory_space=pltpu.HBM),
        out_shape=jax.ShapeDtypeStruct((2, rank, width), F32),
        scratch_shapes=[pltpu.VMEM((2, rank, width), F32), pltpu.SemaphoreType.DMA((2,))],
        name="normalized_panels",
    )(on_chip(arrived), on_chip(image), on_chip(there))


def three_parts(x):
    high = lax.reduce_precision(x, 8, 7)
    middle = lax.reduce_precision(x - high, 8, 7)
    return high.astype(BF16), middle.astype(BF16), (x - high - middle).astype(BF16)


def high_low(gram):
    high = lax.reduce_precision(gram, 8, 7)
    return jnp.concatenate([high.astype(BF16), (gram - high).astype(BF16)], axis=1)


def make(n_x, n_y, n_z):
    share = n_x // 2
    turns = [
        [
            ((i * n_x + j) * 2 + c, (j * n_x + (i + share * c + e) % n_x) * 2 + c)
            for i in range(n_y)
            for j in range(n_x)
            for c in range(2)
        ]
        for e in range(share)
    ]
    flip = [(0, 1), (1, 0)]

    def on_device(weights, preact, panel):
        core = lax.axis_index("core")
        first = core == 0
        _, rank, width_in = panel.shape
        width_row = weights.shape[1]
        w1_own, w2_own = weights[0], weights[1]

        mine, theirs = first_partial(panel, weights)
        traded = lax.ppermute(theirs, "core", flip)
        summed_out = mine + traded

        slopes = 1.0 - jnp.tanh(jnp.where(first, preact[0], preact[1])) ** 2
        slope_1 = slopes[0:1]

        cut = width_row // n_x
        y_at, x_at = lax.axis_index("y"), lax.axis_index("x")
        slope_piece = lax.dynamic_slice(slopes[1:2], (0, x_at * cut), (1, cut), allow_negative_indices=False)
        spot = lax.rem(x_at - y_at + n_x, n_x)
        at_turn = lax.broadcasted_iota(jnp.int32, (1, n_x, cut), 1) == spot
        slope_spread = jnp.where(at_turn, slope_piece[:, None], 0.0).reshape(1, width_row)
        slope_rows = jnp.concatenate([*three_parts(slope_spread), jnp.zeros((8 - 3, width_row), BF16)])

        def piece(turn):
            start = lax.rem(y_at + turn, n_x) * cut
            return lax.dynamic_slice(w2_own, (start, 0), (cut, width_in), allow_negative_indices=False)

        kept = jnp.concatenate([piece(core * share + e) for e in range(share)])
        got = lax.ppermute(jnp.concatenate([piece((1 - core) * share + e) for e in range(share)]), "core", flip)
        rows = jnp.concatenate([jnp.where(first, kept, got), jnp.where(first, got, kept)], axis=1)
        rows = [rows[e * cut : (e + 1) * cut] for e in range(share)]
        here = []
        for e in range(share):
            here.append(lax.ppermute(rows[e], ("y", "x", "core"), turns[e]))
        there = [lax.ppermute(block, "core", flip) for block in here]
        blocks = [jnp.where(first, h, t) for h, t in zip(here, there)]
        blocks += [jnp.where(first, t, h) for h, t in zip(here, there)]
        w2 = jnp.concatenate(blocks)
        w1_other = lax.ppermute(w1_own, "core", flip)
        w1, w2 = lax.optimization_barrier((jnp.concatenate([w1_own, w1_other], axis=1), w2))

        image = None
        for iteration in range(ITERS):
            if iteration == 0:
                arrived = to_all(summed_out.astype(BF16), "x", n_x)
                forward = (slope_1 * total(arrived)).astype(BF16)
            else:
                partial_out = dot_t(image, w1).astype(BF16)
                message = jnp.concatenate([partial_out, high_low(dot_t(image, image))], axis=1)
                arrived = to_all(message, "x", n_x)
                forward = normalized_forward(arrived, slope_1, width_row)
            spread = to_all(forward, "z", n_z)
            spread = jnp.moveaxis(spread, 0, 1).reshape(rank, n_z * width_row)
            partial_out = dot_t(spread, w2).astype(BF16)
            if iteration == 0:
                arrived = to_all(jnp.concatenate([partial_out, slope_rows]), "y", n_y)
                slope_2 = total(arrived[:, rank:]).sum(axis=0, keepdims=True)
                arrived = arrived[:, :rank]
            else:
                arrived = to_all(partial_out, "y", n_y)
            forward = (slope_2 * total(arrived)).astype(BF16)
            weighted = (slope_2 * forward.astype(F32)).astype(BF16)
            partial_in = dot_n(weighted, w2).astype(BF16)
            blocks = jnp.moveaxis(partial_in.reshape(rank, n_z, width_row), 1, 0)
            summed = total(exchange(blocks, "z")).astype(BF16)
            if iteration == ITERS - 1:
                summed = jnp.concatenate([summed, lax.ppermute(summed[:8], "core", flip)])
            cotangent = total(to_all(summed, "x", n_x)[:, :rank]).astype(BF16)
            weighted = (slope_1 * cotangent.astype(F32)).astype(BF16)
            partial_in = dot_n(weighted, w1).astype(BF16)
            groups = rank // 8
            cuts = n_y * n_z // groups
            length = 2 * width_in // cuts
            pieces = partial_in.reshape(groups, 8, cuts, length)
            pieces = jnp.moveaxis(pieces, 2, 1).reshape(groups * cuts, 8, length)
            piece = total(exchange(pieces, ("y", "z"))).astype(BF16)
            image = to_all(piece, ("y", "z"), groups * cuts).reshape(groups, cuts, 8, length)
            image = jnp.moveaxis(image, 1, 2).reshape(rank, 2 * width_in)
        there = lax.ppermute(image[:, width_in:], "core", flip)
        arrived = to_all(high_low(dot_t(image, image)), ("x", "core"), 2 * n_x)
        return normalized_panels(arrived, image, there)

    return on_device


def solution(mesh):
    n_x, n_y, n_z = 4, 4, 8
    fine = Mesh(mesh.devices.reshape(n_y, n_z, n_x, 2), ("y", "z", "x", "core"))
    on_device = make(n_x, n_y, n_z)

    return jax.shard_map(
        on_device,
        mesh=fine,
        in_specs=(P(None, ("y", "z"), ("x", "core")), P(None, None, ("y", "z")), P(None, None, ("x", "core"))),
        out_specs=P(None, None, ("x", "core")),
        check_vma=False,
    )
```

```python
import jax
import jax.numpy as jnp
from jax import lax
from jax.experimental import pallas as pl
from jax.experimental.pallas import tpu as pltpu
from jax.sharding import Mesh, PartitionSpec as P


WIDTH = 8192
ITERS = 2
BF16 = jnp.bfloat16
F32 = jnp.float32
WHOLE = pl.BlockSpec(memory_space=pltpu.VMEM)


def on_chip(x):
    return pltpu.with_memory_space_constraint(x, pltpu.VMEM)


def dot_t(a, w):
    return lax.dot_general(a, w, (((1,), (1,)), ((), ())), preferred_element_type=F32)


def dot_n(a, w):
    return lax.dot_general(a, w, (((1,), (0,)), ((), ())), preferred_element_type=F32)


def exchange(tiles, axis):
    return lax.all_to_all(tiles, axis, split_axis=0, concat_axis=0, tiled=True)


def to_all(x, axis, count):
    return exchange(jnp.broadcast_to(x[None], (count, *x.shape)), axis)


def total(tiles):
    return jnp.sum(tiles.astype(F32), axis=0)


def inverse_factors(grams):
    n = grams[0].shape[0]
    count = n // 8
    rows = lax.broadcasted_iota(jnp.int32, (n, n), 0)
    cols = lax.broadcasted_iota(jnp.int32, (n, n), 1)
    eye = (rows == cols).astype(F32)
    row_of = lax.broadcasted_iota(jnp.int32, (8, 2 * n), 0)
    many, across = [], []
    for gram in grams:
        gram = gram * (1.0 / WIDTH)
        diagonal = gram * eye
        down = 1.0 / jnp.sqrt(jnp.sum(diagonal, axis=1, keepdims=True))
        across.append(1.0 / jnp.sqrt(jnp.sum(diagonal, axis=0, keepdims=True)))
        both = jnp.concatenate([eye, gram * down * across[-1]], axis=1)
        many.append([both[8 * i : 8 * i + 8] for i in range(count)])

    def columns_of(blocks, k):
        return [
            {i: jnp.broadcast_to(blocks[i][:, n + 8 * k + t : n + 8 * k + t + 1], (8, 2 * n)) for i in range(k, count)}
            for t in range(8)
        ]

    def step(blocks, columns, scale, k, t):
        live = range(k, count)
        first, second = columns[t], columns[t + 1]
        a, b, d = first[k][t : t + 1], second[k][t : t + 1], second[k][t + 1 : t + 2]
        over_a, over_next = 1.0 / a, a * (1.0 / (a * d - b * b))
        ratio = b * over_a
        second = {i: second[i] - first[i] * ratio for i in live}
        first = dict(first)
        first[k] = jnp.where(row_of > t, first[k], 0.0)
        second[k] = jnp.where(row_of > t + 1, second[k], 0.0)
        for u in range(t + 2, 8):
            entry = columns[u][k][t : t + 1]
            entry_next = (columns[u][k][t + 1 : t + 2] - entry * ratio) * over_next
            entry = entry * over_a
            for i in live:
                columns[u][i] = columns[u][i] - first[i] * entry - second[i] * entry_next
        row = blocks[k][t : t + 1] * over_a
        row_next = (blocks[k][t + 1 : t + 2] - b * row) * over_next
        for i in live:
            blocks[i] = blocks[i] - first[i] * row - second[i] * row_next
        return jnp.where(row_of == t, over_a, jnp.where(row_of == t + 1, over_next, scale))

    done = [[] for _ in many]
    for k in range(count):
        columns = [columns_of(blocks, k) for blocks in many]
        scales = [jnp.zeros((8, 2 * n), F32) for _ in many]
        for t in range(0, 8, 2):
            for g, blocks in enumerate(many):
                scales[g] = step(blocks, columns[g], scales[g], k, t)
        for g, blocks in enumerate(many):
            done[g].append(blocks[k] * jnp.sqrt(scales[g]))
    return [jnp.concatenate(d, axis=0)[:, :n] * s for d, s in zip(done, across)]


def exact_dot(a, b):
    return lax.dot_general(
        a, b, (((1,), (0,)), ((), ())), precision=lax.Precision.HIGHEST, preferred_element_type=F32
    )


def gram_of_parts(parts_ref, start, rank):
    parts = [parts_ref[i, :, start : start + 2 * rank].astype(F32) for i in range(parts_ref.shape[0])]
    summed = parts[0]
    for part in parts[1:]:
        summed = summed + part
    return summed[:, :rank] + summed[:, rank:]


def first_partial(panel, weights):
    inputs, rank, width = panel.shape
    rows = weights.shape[1]

    def kernel(panel_ref, weights_ref, mine_ref, theirs_ref, panel_here, block_here, sems):
        panel_copy = pltpu.make_async_copy(panel_ref, panel_here, sems.at[0])
        half = rows // 2
        block_copies = [
            pltpu.make_async_copy(
                weights_ref.at[0, pl.ds(i * half, half)], block_here.at[pl.ds(i * half, half)], sems.at[1 + i]
            )
            for i in range(2)
        ]
        panel_copy.start()
        for copy in block_copies:
            copy.start()
        panel_copy.wait()
        core = lax.axis_index("core")
        for i, copy in enumerate(block_copies):
            copy.wait()
            at = slice(i * half, (i + 1) * half)
            block = block_here[at]
            mine_ref[:, at] = dot_t(panel_here[pl.ds(core, 1)][0], block)
            theirs_ref[:, at] = dot_t(panel_here[pl.ds(1 - core, 1)][0], block)

    return pl.pallas_call(
        kernel,
        in_specs=[pl.BlockSpec(memory_space=pltpu.HBM)] * 2,
        out_specs=[WHOLE] * 2,
        out_shape=[pltpu.VMEM((rank, rows), F32)] * 2,
        scratch_shapes=[
            pltpu.VMEM((inputs, rank, width), BF16),
            pltpu.VMEM((rows, width), BF16),
            pltpu.SemaphoreType.DMA((3,)),
        ],
        name="first_partial",
    )(panel, weights)


def normalized_forward(arrived, slope, width):
    count, rank, _ = arrived.shape

    def kernel(arrived_ref, slope_ref, out_ref):
        (inverse,) = inverse_factors([gram_of_parts(arrived_ref, width, rank)])
        summed = arrived_ref[0, :, :width].astype(F32)
        for i in range(1, count):
            summed = summed + arrived_ref[i, :, :width].astype(F32)
        out_ref[...] = (slope_ref[...] * exact_dot(inverse, summed)).astype(BF16)

    return pl.pallas_call(
        kernel,
        in_specs=[WHOLE] * 2,
        out_specs=WHOLE,
        out_shape=pltpu.VMEM((rank, width), BF16),
        name="normalized_forward",
    )(on_chip(arrived), on_chip(slope))


def normalized_panels(arrived, image, there):
    rank, width = there.shape

    def times(inverse, panel):
        high = inverse.astype(BF16)
        rest = inverse - high.astype(F32)
        middle = rest.astype(BF16)
        low = (rest - middle.astype(F32)).astype(BF16)
        products = dot_n(jnp.concatenate([high, middle, low]), panel)
        return products[:rank] + (products[rank : 2 * rank] + products[2 * rank :])

    def kernel(arrived_ref, image_ref, there_ref, out_ref, result, sems):
        here_at = lax.axis_index("core")
        inverses = []
        for b in (here_at, 1 - here_at):
            gram = arrived_ref[pl.ds(b, 1)][0].astype(F32)
            for i in range(2, arrived_ref.shape[0], 2):
                gram = gram + arrived_ref[pl.ds(i + b, 1)][0].astype(F32)
            inverses.append(gram[:, :rank] + gram[:, rank:])
        inverses = inverse_factors(inverses)
        result[0] = times(inverses[0], image_ref[:, :width])
        first = pltpu.make_async_copy(result.at[0], out_ref.at[here_at], sems.at[0])
        first.start()
        result[1] = times(inverses[1], there_ref[...])
        second = pltpu.make_async_copy(result.at[1], out_ref.at[1 - here_at], sems.at[1])
        second.start()
        first.wait()
        second.wait()

    return pl.pallas_call(
        kernel,
        in_specs=[WHOLE] * 3,
        out_specs=pl.BlockSpec(memory_space=pltpu.HBM),
        out_shape=jax.ShapeDtypeStruct((2, rank, width), F32),
        scratch_shapes=[pltpu.VMEM((2, rank, width), F32), pltpu.SemaphoreType.DMA((2,))],
        name="normalized_panels",
    )(on_chip(arrived), on_chip(image), on_chip(there))


def three_parts(x):
    high = lax.reduce_precision(x, 8, 7)
    middle = lax.reduce_precision(x - high, 8, 7)
    return high.astype(BF16), middle.astype(BF16), (x - high - middle).astype(BF16)


def high_low(gram):
    high = lax.reduce_precision(gram, 8, 7)
    return jnp.concatenate([high.astype(BF16), (gram - high).astype(BF16)], axis=1)


def make(n_x, n_y, n_z):
    share = n_x // 2
    turns = [
        [
            ((i * n_x + j) * 2 + c, (j * n_x + (i + share * c + e) % n_x) * 2 + c)
            for i in range(n_y)
            for j in range(n_x)
            for c in range(2)
        ]
        for e in range(share)
    ]
    flip = [(0, 1), (1, 0)]

    def on_device(weights, preact, panel):
        core = lax.axis_index("core")
        first = core == 0
        _, rank, width_in = panel.shape
        width_row = weights.shape[1]
        w1_own, w2_own = weights[0], weights[1]

        mine, theirs = first_partial(panel, weights)
        traded = lax.ppermute(theirs, "core", flip)
        summed_out = mine + traded

        slopes = 1.0 - jnp.tanh(jnp.where(first, preact[0], preact[1])) ** 2
        slope_1 = slopes[0:1]

        cut = width_row // n_x
        y_at, x_at = lax.axis_index("y"), lax.axis_index("x")
        slope_piece = lax.dynamic_slice(slopes[1:2], (0, x_at * cut), (1, cut), allow_negative_indices=False)
        spot = lax.rem(x_at - y_at + n_x, n_x)
        at_turn = lax.broadcasted_iota(jnp.int32, (1, n_x, cut), 1) == spot
        slope_spread = jnp.where(at_turn, slope_piece[:, None], 0.0).reshape(1, width_row)
        slope_rows = jnp.concatenate([*three_parts(slope_spread), jnp.zeros((8 - 3, width_row), BF16)])

        def piece(turn):
            start = lax.rem(y_at + turn, n_x) * cut
            return lax.dynamic_slice(w2_own, (start, 0), (cut, width_in), allow_negative_indices=False)

        kept = jnp.concatenate([piece(core * share + e) for e in range(share)])
        got = lax.ppermute(jnp.concatenate([piece((1 - core) * share + e) for e in range(share)]), "core", flip)
        rows = jnp.concatenate([jnp.where(first, kept, got), jnp.where(first, got, kept)], axis=1)
        rows = [rows[e * cut : (e + 1) * cut] for e in range(share)]
        here = []
        for e in range(share):
            here.append(lax.ppermute(rows[e], ("y", "x", "core"), turns[e]))
        there = [lax.ppermute(block, "core", flip) for block in here]
        blocks = [jnp.where(first, h, t) for h, t in zip(here, there)]
        blocks += [jnp.where(first, t, h) for h, t in zip(here, there)]
        w2 = jnp.concatenate(blocks)
        w1_other = lax.ppermute(w1_own, "core", flip)
        w1, w2 = lax.optimization_barrier((jnp.concatenate([w1_own, w1_other], axis=1), w2))

        image = None
        for iteration in range(ITERS):
            if iteration == 0:
                arrived = to_all(summed_out.astype(BF16), "x", n_x)
                forward = (slope_1 * total(arrived)).astype(BF16)
            else:
                partial_out = dot_t(image, w1).astype(BF16)
                message = jnp.concatenate([partial_out, high_low(dot_t(image, image))], axis=1)
                arrived = to_all(message, "x", n_x)
                forward = normalized_forward(arrived, slope_1, width_row)
            spread = to_all(forward, "z", n_z)
            spread = jnp.moveaxis(spread, 0, 1).reshape(rank, n_z * width_row)
            partial_out = dot_t(spread, w2).astype(BF16)
            if iteration == 0:
                arrived = to_all(jnp.concatenate([partial_out, slope_rows]), "y", n_y)
                slope_2 = total(arrived[:, rank:]).sum(axis=0, keepdims=True)
                arrived = arrived[:, :rank]
            else:
                arrived = to_all(partial_out, "y", n_y)
            forward = (slope_2 * total(arrived)).astype(BF16)
            weighted = (slope_2 * forward.astype(F32)).astype(BF16)
            partial_in = dot_n(weighted, w2).astype(BF16)
            blocks = jnp.moveaxis(partial_in.reshape(rank, n_z, width_row), 1, 0)
            summed = total(exchange(blocks, "z")).astype(BF16)
            cotangent = total(to_all(summed, "x", n_x)).astype(BF16)
            weighted = (slope_1 * cotangent.astype(F32)).astype(BF16)
            partial_in = dot_n(weighted, w1).astype(BF16)
            groups = rank // 8
            cuts = n_y * n_z // groups
            length = 2 * width_in // cuts
            pieces = partial_in.reshape(groups, 8, cuts, length)
            pieces = jnp.moveaxis(pieces, 2, 1).reshape(groups * cuts, 8, length)
            piece = total(exchange(pieces, ("y", "z"))).astype(BF16)
            image = to_all(piece, ("y", "z"), groups * cuts).reshape(groups, cuts, 8, length)
            image = jnp.moveaxis(image, 1, 2).reshape(rank, 2 * width_in)
        there = lax.ppermute(image[:, width_in:], "core", flip)
        arrived = to_all(high_low(dot_t(image, image)), ("x", "core"), 2 * n_x)
        return normalized_panels(arrived, image, there)

    return on_device


def solution(mesh):
    n_x, n_y, n_z = 4, 4, 8
    fine = Mesh(mesh.devices.reshape(n_y, n_z, n_x, 2), ("y", "z", "x", "core"))
    on_device = make(n_x, n_y, n_z)

    return jax.shard_map(
        on_device,
        mesh=fine,
        in_specs=(P(None, ("y", "z"), ("x", "core")), P(None, None, ("y", "z")), P(None, None, ("x", "core"))),
        out_specs=P(None, None, ("x", "core")),
        check_vma=False,
    )
```
